32 devices in a mesh: batch: 16 (over z, y, core), rows: 2 (over x).
Axes of the slice: x: 2, y: 2, z: 4, core: 2. Of those that a mesh axis runs over, the one named last changes fastest.
Arguments:
- block_input: bfloat16 [16, 16, 64, 384], P('batch', 'rows'), may hold values from -6 to 6
- output_grad: bfloat16 [16, 16, 64, 768], P('batch', 'rows'), may hold values from -6 to 6
- conv_weight: float32 [384, 1152], P(None, 'batch'), may hold values from -12 to 12
- conv_gain: float32 [384], replicated, may hold values from 0.1 to 1.9
- conv_momentum: float32 [384, 1152], P(None, 'batch'), may hold values from -0.6 to 0.6
- proj_weight: float32 [768, 384], P(None, 'batch'), may hold values from -12 to 12
- proj_gain: float32 [768], replicated, may hold values from 0.1 to 1.9
- proj_momentum: float32 [768, 384], P(None, 'batch'), may hold values from -0.6 to 0.6
Outputs:
- input_grad: bfloat16 [16, 16, 64, 384], P('batch', 'rows')
- new_conv_weight: float32 [384, 1152], P(None, 'batch')
- new_conv_momentum: float32 [384, 1152], P(None, 'batch')
- new_proj_weight: float32 [768, 384], P(None, 'batch')
- new_proj_momentum: float32 [768, 384], P(None, 'batch')
The draws below stay inside these ranges and needn't reach their ends.
All inputs are finite; a program needn't handle non-finite values.
Results may differ from the reference program's by a relative error of at most 0.0031.
The reference program's roundings to bfloat16 on the way (of `standard`, `activated`, `hidden` and `pre_grad`) count: a program that leaves them out, or rounds other values in their place, can miss the bound.
Values may be sent and summed in bfloat16 or wider, within the bound.
A program may use at most 64 MiB of HBM per device.

```python
import math
import jax
import jax.numpy as jnp
from jax import lax

CH = 384
GW = 128
OUT = 768
COLS = 64
IMAGES = 16
MAP_ROWS = 16


def scaled_rows(key, row_count, col_count):
    key_scale, key_body = jax.random.split(key)
    log_scale = jax.random.uniform(key_scale, (row_count, 1), jnp.float32, math.log(0.3), math.log(3.0))
    values = jax.random.truncated_normal(key_body, -4.0, 4.0, (row_count, col_count), jnp.float32)
    return jnp.exp(log_scale) * values


def draw_conv_weight(key, part):
    return scaled_rows(jax.random.fold_in(key, 11), CH, 9 * GW)


def draw_proj_weight(key, part):
    return scaled_rows(jax.random.fold_in(key, 23), OUT, CH)


def levels(stream_key, shape, pieces, low, largest):
    def one(axis_at, parts):
        heights = jax.random.uniform(jax.random.fold_in(jax.random.fold_in(stream_key, 6), axis_at), (parts,), jnp.float32, low / len(pieces), largest / len(pieces))
        return jnp.repeat(jnp.exp(heights), shape[axis_at] // parts).reshape((-1,) + (1,) * (len(shape) - axis_at - 1))

    level = one(*pieces[0])
    for cut in pieces[1:]:
        level = level * one(*cut)
    return level


def normal_values(stream_key, dims, width, most, cuts=(), dtype=jnp.bfloat16):
    factor_of = levels(stream_key, dims, cuts, -0.22, 0.18) if cuts else 1.0
    values = jax.random.normal(stream_key, dims, jnp.float32) * width * factor_of
    return jnp.minimum(jnp.maximum(values, -most), most).astype(dtype)


def setup_inputs(seed: int = 0) -> dict:
    arg_keys = jax.random.split(jax.random.key(seed), 9)
    return {
        "block_input": normal_values(arg_keys[0], (IMAGES, MAP_ROWS, COLS, CH), 1.0, 6.0, ((0, 16), (1, 2))),
        "output_grad": normal_values(arg_keys[1], (IMAGES, MAP_ROWS, COLS, OUT), 1.0, 6.0, ((0, 16), (1, 2))),
        "conv_weight": draw_conv_weight(jax.random.fold_in(arg_keys[8], 71), 0),
        "conv_gain": jnp.clip(1.0 + 0.18 * jax.random.normal(arg_keys[3], (CH,), jnp.float32), 0.1, 1.9),
        "conv_momentum": normal_values(arg_keys[4], (CH, 9 * GW), 0.1, 0.6, ((1, 16),), jnp.float32),
        "proj_weight": draw_proj_weight(jax.random.fold_in(arg_keys[8], 71), 0),
        "proj_gain": jnp.clip(1.0 + 0.18 * jax.random.normal(arg_keys[6], (OUT,), jnp.float32), 0.1, 1.9),
        "proj_momentum": normal_values(arg_keys[7], (OUT, CH), 0.1, 0.6, ((1, 16),), jnp.float32),
    }


ws_eps = 0.0001
clip_ratio = 0.05
momentum_rate = 0.9
learn_rate = 1.6
norm_eps = 1e-06

def gelu_slope(values):
    return jax.jvp(jax.nn.gelu, (values,), (jnp.ones_like(values),))[1]

def standardize(weight, gain_row):
    center = lax.optimization_barrier(jnp.mean(weight, axis=1, keepdims=True))
    centered = weight - center
    spread = lax.optimization_barrier(jnp.sum(centered * centered, axis=1))
    factor = lax.rsqrt(spread + ws_eps)
    standard = ((gain_row * factor)[:, None] * centered).astype(jnp.bfloat16)
    return (standard, centered, factor)

def apply_update(weight, momentum, raw_grad, weight_sq, grad_sq):
    clip_scale = jnp.minimum(1.0, clip_ratio * jnp.sqrt(weight_sq) * lax.rsqrt(grad_sq + norm_eps))
    clipped = raw_grad * clip_scale[:, None]
    new_momentum = momentum_rate * momentum + clipped
    return (weight - learn_rate * (clipped + momentum_rate * new_momentum), new_momentum)

def update(weight, gain_row, momentum, centered, factor, grad_std):
    fan_in = weight.shape[1]
    grad_sum = lax.optimization_barrier(jnp.sum(grad_std, axis=1))
    grad_proj = lax.optimization_barrier(jnp.sum(grad_std * centered, axis=1))
    coef_one = gain_row * factor
    coef_two = gain_row * factor ** 3 * grad_proj
    raw_grad = coef_one[:, None] * (grad_std - (grad_sum / fan_in)[:, None]) - coef_two[:, None] * centered
    weight_sq = lax.optimization_barrier(jnp.sum(weight * weight, axis=1))
    grad_sq = lax.optimization_barrier(jnp.sum(raw_grad * raw_grad, axis=1))
    return apply_update(weight, momentum, raw_grad, weight_sq, grad_sq)

def reference(block_input, output_grad, conv_weight, conv_gain, conv_momentum, proj_weight, proj_gain, proj_momentum):
    conv_std, conv_cent, conv_factor = standardize(conv_weight, conv_gain)
    proj_std, proj_cent, proj_factor = standardize(proj_weight, proj_gain)
    groups = CH // GW
    kernel = conv_std.reshape(groups, GW, 9, GW).astype(jnp.float32)
    image_count = block_input.shape[0]
    map_rows = block_input.shape[1]
    map_cols = block_input.shape[2]
    pixels = map_rows * map_cols

    def image_step(carry, inputs):
        conv_acc, proj_acc = carry
        image, cotangent = inputs
        activated = jax.nn.gelu(image.astype(jnp.float32)).astype(jnp.bfloat16)
        padded = jnp.pad(activated, ((1, 1), (1, 1), (0, 0)))
        patch_list = []
        pre_act = jnp.zeros((pixels, groups, GW), jnp.float32)
        for position in range(9):
            top = position // 3
            left = position % 3
            patch = padded[top:top + map_rows, left:left + map_cols].reshape(pixels, groups, GW).astype(jnp.float32)
            patch_list.append(patch)
            pre_act = pre_act + jnp.einsum('pgi,goi->pgo', patch, kernel[:, :, position, :])
        pre_flat = pre_act.reshape(pixels, CH)
        hidden = jax.nn.gelu(pre_flat).astype(jnp.bfloat16)
        upstream = cotangent.reshape(pixels, OUT)
        hidden_grad = jnp.dot(upstream, proj_std, preferred_element_type=jnp.float32)
        pre_grad = (hidden_grad * gelu_slope(pre_flat)).astype(jnp.bfloat16)
        proj_acc = proj_acc + jnp.einsum('po,pi->oi', upstream.astype(jnp.float32), hidden.astype(jnp.float32))
        grad_groups = pre_grad.reshape(pixels, groups, GW).astype(jnp.float32)
        conv_terms = jnp.stack([jnp.einsum('pgi,pgo->goi', patch, grad_groups) for patch in patch_list], axis=2)
        conv_acc = conv_acc + conv_terms.reshape(CH, 9 * GW)
        grad_pad = jnp.pad(pre_grad.reshape(map_rows, map_cols, CH), ((1, 1), (1, 1), (0, 0)))
        act_grad = jnp.zeros((pixels, groups, GW), jnp.float32)
        for position in range(9):
            top = 2 - position // 3
            left = 2 - position % 3
            piece = grad_pad[top:top + map_rows, left:left + map_cols].reshape(pixels, groups, GW).astype(jnp.float32)
            act_grad = act_grad + jnp.einsum('pgo,goi->pgi', piece, kernel[:, :, position, :])
        slope = gelu_slope(image.astype(jnp.float32))
        input_grad = (act_grad.reshape(map_rows, map_cols, CH) * slope).astype(jnp.bfloat16)
        return ((conv_acc, proj_acc), input_grad)
    start = (jnp.zeros((CH, 9 * GW), jnp.float32), jnp.zeros((OUT, CH), jnp.float32))
    (conv_acc, proj_acc), input_grad = lax.scan(image_step, start, (block_input, output_grad))
    conv_grad = conv_acc / image_count
    proj_grad = proj_acc / image_count
    new_conv_weight, new_conv_momentum = update(conv_weight, conv_gain, conv_momentum, conv_cent, conv_factor, conv_grad)
    new_proj_weight, new_proj_momentum = update(proj_weight, proj_gain, proj_momentum, proj_cent, proj_factor, proj_grad)
    return (input_grad, new_conv_weight, new_conv_momentum, new_proj_weight, new_proj_momentum)
```

```python
import functools
import math

import jax
import jax.numpy as jnp
from jax import lax
from jax.experimental import pallas as pl
from jax.experimental.pallas import tpu as pltpu
from jax.sharding import PartitionSpec as P

ws_eps = 0.0001
clip_ratio = 0.05
momentum_rate = 0.9
learn_rate = 1.6
norm_eps = 1e-06

F32 = jnp.float32
BF16 = jnp.bfloat16
MESH = pl.DeviceIdType.MESH
TAPS = 3
C0 = math.sqrt(2.0 / math.pi)
C1 = 0.044715


def gelu_parts(x):
    t = jnp.tanh(C0 * (x + C1 * (x * x * x)))
    half = 0.5 * (1.0 + t)
    slope = half + (0.5 * C0) * x * (1.0 - t * t) * (1.0 + (3.0 * C1) * (x * x))
    return x * half, slope


def dot_nn(a, b):
    return jnp.dot(a, b, preferred_element_type=F32)


def dot_nt(a, b):
    return lax.dot_general(a, b, (((1,), (1,)), ((), ())), preferred_element_type=F32)


def dot_tn(a, b):
    return lax.dot_general(a, b, (((0,), (0,)), ((), ())), preferred_element_type=F32)


LANE = 128


class Plan:
    def __init__(self, n, ch, out, nc, np_):
        nb = n.bit_length() - 1
        assert 2**nb == n and nb >= 1
        self.n, self.nc, self.np_ = n, nc, np_
        self.nz = 2 ** (nb // 2)
        self.nm = n // 2 // self.nz
        self.half = n // 2
        self.ch, self.out = ch, out
        self.nblk = out // ch
        self.pieces = ch // LANE
        cut = self.pieces // 2
        rest = self.pieces - cut
        self.sets = (
            [("q", k) for k in range(cut)] + [("c", k) for k in range(rest)],
            [("q", k) for k in range(cut, self.pieces)] + [("c", k) for k in range(rest, self.pieces)],
        )
        self.tiles = tuple([t for chunk in one for t in self.tiles_of(chunk)] for one in self.sets)
        self.wide = max(len(t) for t in self.tiles)
        assert self.wide <= 5
        self.proj_tiles = tuple(sum(which for which, _ in one) for one in self.tiles)

    def tiles_of(self, chunk):
        kind, k = chunk
        if kind == "c":
            return [(0, k * LANE)]
        return [(1, b * self.ch + k * LANE) for b in range(self.nblk)]

    def count_of(self, which):
        return self.np_ if which else self.nc

    def chunk_rows(self, kind):
        return self.nc if kind == "c" else self.nblk * self.np_

    def slot(self, d):
        return (d % 2 * self.nm + d // 2 % self.nm) * self.nz + d // 2 // self.nm

    def place(self, me):
        return me % 2, me // 2 % self.nm, me // 2 // self.nm

    def batch(self, c, m, z):
        return (z * self.nm + m) * 2 + c


def send(src, dst, sems, at, where):
    return pltpu.make_async_remote_copy(
        src_ref=src, dst_ref=dst, send_sem=sems[0].at[at], recv_sem=sems[1].at[at],
        device_id=where, device_id_type=MESH,
    )


def greet(plan):
    me = lax.axis_index("batch")
    r = lax.axis_index("rows")
    c, m, z = plan.place(me)
    n = plan.n
    barrier = pltpu.get_barrier_semaphore()
    for d in range(1, n):
        pl.semaphore_signal(barrier, inc=1, device_id={"batch": (me + d) % n}, device_id_type=MESH)
    for j in range(plan.nm):
        to = plan.batch(c, (m + j) % plan.nm, z)
        pl.semaphore_signal(barrier, inc=1, device_id={"batch": to, "rows": 1 - r}, device_id_type=MESH)


def greet_wait(plan):
    pl.semaphore_wait(pltpu.get_barrier_semaphore(), plan.n - 1 + plan.nm)


def push_all(plan, me, src, slots, sems):
    n = plan.n
    copies = []
    for d in range(1, n):
        copy = send(src, slots.at[me], sems, d - 1, {"batch": (me + d) % n})
        copy.start()
        copies.append(copy)
    slots[me] = src[...]
    return copies


def counts_of(plan, r):
    row = lax.broadcasted_iota(jnp.int32, (8, LANE), 0)
    first = jnp.where(r == 0, plan.proj_tiles[0], plan.proj_tiles[1])
    return jnp.where(row < first, float(plan.np_), float(plan.nc))


def merged(plan, slots, cnt):
    w = plan.wide
    total = slots[0]
    for i in range(1, plan.n):
        total = total + slots[i]
    mean = total[0:8] / (plan.n * cnt)
    between = None
    for i in range(plan.n):
        off = slots[i, 0:8] / cnt - mean
        term = cnt * (off * off)
        between = term if between is None else between + term
    return total, mean[0:w], total[w : 2 * w] + between[0:w]


def by_half(r, fn):
    for rr in range(2):
        @pl.when(r == rr)
        def _(rr=rr):
            fn(rr)


def gather_kernel(plan, edge_x, edge_u, wc_ref, wp_ref, gc_ref, gp_ref, x_ref, u_ref,
                  fc_ref, fq_ref, stat_ref, hx_ref, hu_ref,
                  src, slots, s_send, s_recv, z_send, z_recv, m_send, m_recv,
                  d_send, d_recv, h_send, h_recv):
    me = lax.axis_index("batch")
    r = lax.axis_index("rows")
    c, m, z = plan.place(me)
    nz, nm, w = plan.nz, plan.nm, plan.wide
    greet(plan)
    w_refs = (wc_ref, wp_ref)
    gain_refs = (gc_ref, gp_ref)
    full = {"c": fc_ref, "q": fq_ref}
    src[...] = jnp.zeros_like(src)

    def local_stats(rr):
        for i, (which, col) in enumerate(plan.tiles[rr]):
            piece = w_refs[which][:, col : col + LANE]
            s = jnp.sum(piece, axis=0, keepdims=True)
            cent = piece - s / piece.shape[0]
            src[i : i + 1] = s
            src[w + i : w + i + 1] = jnp.sum(cent * cent, axis=0, keepdims=True)

    by_half(r, local_stats)
    greet_wait(plan)
    push = push_all(plan, me, src, slots, (s_send, s_recv))
    halos = []
    for at, (ref, out, width) in enumerate(((x_ref, hx_ref, edge_x), (u_ref, hu_ref, edge_u))):
        first = (1 - r) * (ref.shape[0] - width)
        copy = send(ref.at[pl.ds(first, width)], out, (h_send, h_recv), at, {"rows": 1 - r})
        copy.start()
        halos.append(copy)
    for copy in push:
        copy.wait()
    cnt = counts_of(plan, r)
    _, mean, spread = merged(plan, slots, cnt)
    stat_ref[r] = jnp.zeros_like(stat_ref[0])
    stat_ref[r, 0:w] = mean
    stat_ref[r, 8 : 8 + w] = spread
    copy = send(stat_ref.at[r], stat_ref.at[r], (h_send, h_recv), 2, {"rows": 1 - r})
    copy.start()
    halos.append(copy)
    factor = lax.rsqrt(spread + ws_eps)
    slot = (c * nm + m) * nz + z

    def z_copy(k, j, chunk):
        kind, g = chunk
        at = full[kind].at[g, slot]
        return send(at, at, (z_send, z_recv), (k, j - 1), {"batch": plan.batch(c, m, (z + j) % nz)})

    def start_z(rr):
        i = 0
        for k, chunk in enumerate(plan.sets[rr]):
            kind, g = chunk
            for b, (which, col) in enumerate(plan.tiles_of(chunk)):
                count = plan.count_of(which)
                scale = gain_refs[which][col : col + LANE][None] * factor[i : i + 1]
                std = (scale * (w_refs[which][:, col : col + LANE] - mean[i : i + 1])).astype(BF16)
                full[kind][g, slot, b * count : (b + 1) * count] = std
                i += 1
            for j in range(1, nz):
                z_copy(k, j, chunk).start()

    by_half(r, start_z)
    base = (c * nm + m) * nz

    def m_copy(k, j, jx, chunk, rows):
        kind, g = chunk
        at = full[kind].at[g, pl.ds(base, nz)]
        where = {"batch": plan.batch(c, (m + j) % nm, z), "rows": (r + jx) % 2}
        return send(at, at, (m_send, m_recv), (k, jx * nm + j - 1), where)

    peers = [(j, jx) for jx in range(2) for j in range(nm) if (j, jx) != (0, 0)]

    def spread_m(k):
        def fn(rr):
            chunk = plan.sets[rr][k]
            for j in range(1, nz):
                z_copy(k, j, chunk).wait()
            for j, jx in peers:
                m_copy(k, j, jx, chunk, None).start()
        by_half(r, fn)

    def finish_m(k):
        def fn(rr):
            for j, jx in peers:
                m_copy(k, j, jx, plan.sets[rr][k], None).wait_send()
                m_copy(k, j, jx, plan.sets[(rr + jx) % 2][k], None).wait_recv()
        by_half(r, fn)

    def d_copy(k, side):
        kind, g = plan.sets[side][k]
        at = full[kind].at[g, pl.ds(c * plan.half, plan.half)]
        return send(at, at, (d_send, d_recv), (k, side), {"batch": plan.batch(1 - c, m, z)})

    for k in range(plan.pieces):
        spread_m(k)
    for k in range(plan.pieces):
        finish_m(k)
        for side in range(2):
            d_copy(k, side).start()
    for k in range(plan.pieces):
        for side in range(2):
            d_copy(k, side).wait()
    for copy in halos:
        copy.wait()


def reduce_kernel(plan, images, pc_ref, pq_ref, wc_ref, wp_ref, stat_ref, gc_ref, gp_ref,
                  gradc_ref, gradq_ref, coef_ref,
                  dc, dq, ac, aq, mc_, mq, zc, zq, bc, bq, src, slots, gain_s,
                  s_send, s_recv, z_send, z_recv, m_send, m_recv, d_send, d_recv, x_send, x_recv):
    me = lax.axis_index("batch")
    r = lax.axis_index("rows")
    c, m, z = plan.place(me)
    nz, nm, w = plan.nz, plan.nm, plan.wide
    part = {"c": pc_ref, "q": pq_ref}
    got_d = {"c": dc, "q": dq}
    two = {"c": ac, "q": aq}
    got_m = {"c": mc_, "q": mq}
    eight = {"c": bc, "q": bq}
    got_z = {"c": zc, "q": zq}
    grads = {"c": gradc_ref, "q": gradq_ref}
    greet(plan)
    greet_wait(plan)
    order = list(reversed(range(plan.pieces)))

    def d_copy(k, side):
        kind, g = plan.sets[side][k]
        return send(
            part[kind].at[g, pl.ds((1 - c) * plan.half, plan.half)], got_d[kind].at[g],
            (d_send, d_recv), (k, side), {"batch": plan.batch(1 - c, m, z)},
        )

    for k in order:
        for side in range(2):
            d_copy(k, side).start()

    def m_copy(k, j, jx, chunk):
        kind, g = chunk
        to = (m + j) % nm
        return send(
            two[kind].at[g, pl.ds(to * nz, nz)], got_m[kind].at[g, jx * nm + j - 1],
            (m_send, m_recv), (k, jx * nm + j - 1),
            {"batch": plan.batch(c, to, z), "rows": (r + jx) % 2},
        )

    peers = [(j, jx) for jx in (1, 0) for j in reversed(range(nm)) if (j, jx) != (0, 0)]

    def step_m(k):
        for side in range(2):
            d_copy(k, side).wait()

        def fn(rr):
            for j, jx in peers:
                kind, g = plan.sets[(rr + jx) % 2][k]
                first = (m + j) % nm * nz

                def add(i, carry, kind=kind, g=g, first=first):
                    total = part[kind][g, c * plan.half + first + i].astype(F32) + got_d[kind][g, first + i].astype(F32)
                    two[kind][g, first + i] = total.astype(BF16)
                    return carry

                lax.fori_loop(0, nz, add, 0)
                m_copy(k, j, jx, (kind, g)).start()
        by_half(r, fn)

    def z_copy(k, j, chunk):
        kind, g = chunk
        to = (z + j) % nz
        return send(
            eight[kind].at[g, to], got_z[kind].at[g, j - 1],
            (z_send, z_recv), (k, j - 1), {"batch": plan.batch(c, m, to)},
        )

    def sum_m(kind, g, at):
        first = m * nz + at
        total = part[kind][g, c * plan.half + first].astype(F32) + got_d[kind][g, first].astype(F32)
        for i in range(2 * nm - 1):
            total = total + got_m[kind][g, i, at].astype(F32)
        return total

    def step_z(k):
        def fn(rr):
            for j, jx in peers:
                m_copy(k, j, jx, plan.sets[(rr + jx) % 2][k]).wait_send()
                m_copy(k, j, jx, plan.sets[rr][k]).wait_recv()
            kind, g = plan.sets[rr][k]
            for j in range(1, nz):
                to = (z + j) % nz
                eight[kind][g, to] = sum_m(kind, g, to).astype(BF16)
                z_copy(k, j, (kind, g)).start()
            grads[kind][g] = sum_m(kind, g, z)
        by_half(r, fn)

    def x_copy(k, chunk):
        kind, g = chunk
        return send(grads[kind].at[g], grads[kind].at[g], (x_send, x_recv), k, {"rows": 1 - r})

    def finish(k):
        def fn(rr):
            kind, g = plan.sets[rr][k]
            total = grads[kind][g]
            for j in range(1, nz):
                z_copy(k, j, (kind, g)).wait()
                total = total + got_z[kind][g, j - 1].astype(F32)
            grads[kind][g] = total / images
            x_copy(k, (kind, g)).start()
        by_half(r, fn)

    for k in order:
        step_m(k)
    for k in order:
        step_z(k)
    for k in order:
        finish(k)
    w_refs = (wc_ref, wp_ref)
    gain_refs = (gc_ref, gp_ref)
    src[...] = jnp.zeros_like(src)
    gain_s[...] = jnp.zeros_like(gain_s)

    def local_stats(rr):
        i = 0
        for chunk in plan.sets[rr]:
            kind, g = chunk
            for b, (which, col) in enumerate(plan.tiles_of(chunk)):
                count = plan.count_of(which)
                piece = grads[kind][g, b * count : (b + 1) * count]
                cent = w_refs[which][:, col : col + LANE] - stat_ref[rr, i : i + 1]
                s = jnp.sum(piece, axis=0, keepdims=True)
                off = piece - s / count
                src[i : i + 1] = s
                src[w + i : w + i + 1] = jnp.sum(off * off, axis=0, keepdims=True)
                src[2 * w + i : 2 * w + i + 1] = jnp.sum(piece * cent, axis=0, keepdims=True)
                gain_s[i : i + 1] = gain_refs[which][col : col + LANE][None]
                i += 1

    by_half(r, local_stats)
    for copy in push_all(plan, me, src, slots, (s_send, s_recv)):
        copy.wait()
    cnt = counts_of(plan, r)
    total, gmean, gspread = merged(plan, slots, cnt)
    proj = total[2 * w : 3 * w]
    fan = plan.n * cnt[0:w]
    mean = stat_ref[r, 0:w]
    spread = stat_ref[r, 8 : 8 + w]
    factor = lax.rsqrt(spread + ws_eps)
    f2 = factor * factor
    one = gain_s[0:w] * factor
    coef_two = one * f2 * proj
    grad_sq = one * one * jnp.maximum(gspread - f2 * proj * proj * (2.0 - f2 * spread), 0.0)
    weight_sq = spread + fan * (mean * mean)
    clip = jnp.minimum(1.0, clip_ratio * jnp.sqrt(weight_sq) * lax.rsqrt(grad_sq + norm_eps))
    coef_ref[r] = jnp.zeros_like(coef_ref[0])
    coef_ref[r, 0:w] = clip * one
    coef_ref[r, 8 : 8 + w] = gmean
    coef_ref[r, 16 : 16 + w] = clip * coef_two
    last = send(coef_ref.at[r], coef_ref.at[r], (x_send, x_recv), plan.pieces, {"rows": 1 - r})
    last.start()

    def end(rr):
        for k in range(plan.pieces):
            x_copy(k, plan.sets[rr][k]).wait_send()
            x_copy(k, plan.sets[1 - rr][k]).wait_recv()

    by_half(r, end)
    last.wait()


def update_kernel(plan, gradc_ref, gradq_ref, coef_ref, stat_ref, wc_ref, wp_ref, mc_ref, mp_ref,
                  nwc_ref, nwp_ref, nmc_ref, nmp_ref):
    grads = {"c": gradc_ref, "q": gradq_ref}
    for rr in range(2):
        i = 0
        for chunk in plan.sets[rr]:
            kind, g = chunk
            for b, (which, col) in enumerate(plan.tiles_of(chunk)):
                count = plan.count_of(which)
                cols = slice(col, col + LANE)
                w = (wc_ref, wp_ref)[which][:, cols]
                grad = grads[kind][g, b * count : (b + 1) * count]
                clipped = coef_ref[rr, i : i + 1] * (grad - coef_ref[rr, 8 + i : 9 + i]) - coef_ref[
                    rr, 16 + i : 17 + i
                ] * (w - stat_ref[rr, i : i + 1])
                new_m = momentum_rate * (mc_ref, mp_ref)[which][:, cols] + clipped
                (nmc_ref, nmp_ref)[which][:, cols] = new_m
                (nwc_ref, nwp_ref)[which][:, cols] = w - learn_rate * (clipped + momentum_rate * new_m)
                i += 1


def shifted(vals, step, mc):
    rows = vals.shape[0]
    col = lax.broadcasted_iota(jnp.int32, vals.shape, 0)
    if step > 0:
        return jnp.where(col == mc - 1, 0.0, pltpu.roll(vals, rows - 1, 0))
    return jnp.where(col == 0, 0.0, pltpu.roll(vals, 1, 0))


def compute_kernel(plan, mr, mc, gw,
                   x_ref, u_ref, hx_ref, hu_ref, fc_ref, fq_ref,
                   ig_ref, pc_ref, pq_ref,
                   kt, pt, xs, ys, hid, cg, pg):
    n, nc, np_, nblk = plan.n, plan.nc, plan.np_, plan.nblk
    order = [plan.slot(d) for d in range(n)]
    ch = x_ref.shape[1]
    groups = ch // gw
    wide = TAPS * gw
    px = mr * mc
    r = lax.axis_index("rows")
    for d in range(n):
        for p in range(ch // LANE):
            kt[d * nc : (d + 1) * nc, p * LANE : (p + 1) * LANE] = fc_ref[p, order[d]]
            for b in range(nblk):
                at = b * ch + p * LANE
                pt[d * np_ : (d + 1) * np_, at : at + LANE] = fq_ref[
                    p, order[d], b * np_ : (b + 1) * np_
                ]

    def place(at, vals):
        act = gelu_parts(vals)[0].astype(BF16).astype(F32)
        for j in range(TAPS):
            moved = act if j == 1 else shifted(act, j - 1, mc)
            moved = moved.astype(BF16)
            for g in range(groups):
                xs[pl.ds(at, mc), g * wide + j * gw : g * wide + (j + 1) * gw] = moved[
                    :, g * gw : (g + 1) * gw
                ]

    for e in range(2):
        edge = hx_ref[e * mc : (e + 1) * mc].astype(F32)
        place(e * mc, jnp.where(r == 1, edge, 0.0))
        place((mr + 2 + e) * mc, jnp.where(r == 0, edge, 0.0))

    def body(row, carry):
        at = pl.multiple_of(row * mc, mc)
        place(pl.multiple_of(at + 2 * mc, mc), x_ref[pl.ds(at, mc)].astype(F32))
        return carry

    lax.fori_loop(0, mr, body, 0)

    def forward(e, up):
        hg = dot_nt(up, pt[...])
        for g in range(groups):
            acc = None
            for i in range(TAPS):
                term = dot_nn(
                    xs[pl.ds(pl.multiple_of((e + i) * mc, mc), up.shape[0]), g * wide : (g + 1) * wide],
                    kt[i * wide : (i + 1) * wide, g * gw : (g + 1) * gw],
                )
                acc = term if acc is None else acc + term
            h, slope = gelu_parts(acc)
            hid[pl.ds(pl.multiple_of(e * mc, mc), up.shape[0]), g * gw : (g + 1) * gw] = h.astype(BF16)
            grad = (hg[:, g * gw : (g + 1) * gw] * slope).astype(BF16).astype(F32)
            for q in range(up.shape[0] // mc):
                here = grad[q * mc : (q + 1) * mc]
                for j in range(TAPS):
                    moved = here if j == 1 else shifted(here, 1 - j, mc)
                    ys[pl.ds(pl.multiple_of((e + q) * mc, mc), mc), g * wide + j * gw : g * wide + (j + 1) * gw] = moved.astype(BF16)

    edge = hu_ref[...].astype(F32)
    forward(0, jnp.where(r == 1, edge, 0.0).astype(BF16))
    forward(mr + 1, jnp.where(r == 0, edge, 0.0).astype(BF16))
    many = 2 if mr % 2 == 0 else 1

    def fwd(t, carry):
        up = u_ref[pl.ds(pl.multiple_of(t * many * mc, mc), many * mc)]
        forward(1 + t * many, up)
        return carry

    lax.fori_loop(0, mr // many, fwd, 0)

    pg[...] = dot_tn(hid[mc : mc + px], u_ref[...])
    for g in range(groups):
        own = ys[mc : mc + px, g * wide + gw : g * wide + 2 * gw]
        for i in range(TAPS):
            cg[i * wide : (i + 1) * wide, g * gw : (g + 1) * gw] = dot_tn(
                xs[(1 + i) * mc : (1 + i) * mc + px, g * wide : (g + 1) * wide], own
            )
    for d in range(n):
        for p in range(ch // LANE):
            pc_ref[p, order[d]] = cg[
                d * nc : (d + 1) * nc, p * LANE : (p + 1) * LANE
            ].astype(BF16)
            for b in range(nblk):
                at = b * ch + p * LANE
                pq_ref[p, order[d], b * np_ : (b + 1) * np_] = pg[
                    d * np_ : (d + 1) * np_, at : at + LANE
                ].astype(BF16)

    def back(t, carry):
        at = pl.multiple_of(t * many * mc, mc)
        for g in range(groups):
            acc = None
            for i in range(TAPS):
                for j in range(TAPS):
                    term = dot_nt(
                        ys[pl.ds(pl.multiple_of(at + (2 - i) * mc, mc), many * mc), g * wide + j * gw : g * wide + (j + 1) * gw],
                        kt[i * wide + j * gw : i * wide + (j + 1) * gw, g * gw : (g + 1) * gw],
                    )
                    acc = term if acc is None else acc + term
            slope = gelu_parts(x_ref[pl.ds(at, many * mc), g * gw : (g + 1) * gw].astype(F32))[1]
            ig_ref[pl.ds(at, many * mc), g * gw : (g + 1) * gw] = (acc * slope).astype(BF16)
        return carry

    lax.fori_loop(0, mr // many, back, 0)


def local(n, nrows, block_input, output_grad, conv_weight, conv_gain, conv_momentum,
          proj_weight, proj_gain, proj_momentum):
    assert nrows == 2
    _, mr, mc, ch = block_input.shape
    out = output_grad.shape[3]
    nc = conv_weight.shape[1]
    np_ = proj_weight.shape[1]
    gw = nc * n // (TAPS * TAPS)
    plan = Plan(n, ch, out, nc, np_)
    nz, nm, half, pieces = plan.nz, plan.nm, plan.half, plan.pieces
    px = mr * mc
    rq = plan.chunk_rows("q")

    wc, wp, mc_, mp = conv_weight.T, proj_weight.T, conv_momentum.T, proj_momentum.T
    gc, gp = conv_gain, proj_gain
    x = block_input.reshape(px, ch)
    u = output_grad.reshape(px, out)
    vmem = pl.BlockSpec(memory_space=pltpu.VMEM)
    sdt = jax.ShapeDtypeStruct
    dma = pltpu.SemaphoreType.DMA

    def pair(shape):
        return [dma(shape), dma(shape)]

    def both(*lead, dtype=BF16):
        return [pltpu.VMEM((pieces, *lead, nc, LANE), dtype), pltpu.VMEM((pieces, *lead, rq, LANE), dtype)]

    whole = (sdt((pieces, n, nc, LANE), BF16), sdt((pieces, n, rq, LANE), BF16))
    fc, fq, stat, hx, hu = pl.pallas_call(
        functools.partial(gather_kernel, plan, 2 * mc, mc),
        out_shape=whole + (
            sdt((2, 16, LANE), F32),
            sdt((2 * mc, ch), BF16),
            sdt((mc, out), BF16),
        ),
        in_specs=[vmem] * 6,
        out_specs=(vmem,) * 5,
        scratch_shapes=[pltpu.VMEM((16, LANE), F32), pltpu.VMEM((n, 16, LANE), F32)]
        + pair((n - 1,)) + pair((pieces, max(nz - 1, 1))) + pair((pieces, 2 * nm - 1))
        + pair((pieces, 2)) + pair((3,)),
        compiler_params=pltpu.CompilerParams(collective_id=0, has_side_effects=True),
        name="gather",
    )(wc, wp, gc, gp, x, u)
    ig, pc, pq = pl.pallas_call(
        functools.partial(compute_kernel, plan, mr, mc, gw),
        out_shape=(sdt((px, ch), BF16),) + whole,
        in_specs=[vmem] * 6,
        out_specs=(vmem,) * 3,
        scratch_shapes=[
            pltpu.VMEM((n * nc, ch), BF16),
            pltpu.VMEM((n * np_, out), BF16),
            pltpu.VMEM(((mr + 4) * mc, TAPS * ch), BF16),
            pltpu.VMEM(((mr + 2) * mc, TAPS * ch), BF16),
            pltpu.VMEM(((mr + 2) * mc, ch), BF16),
            pltpu.VMEM((n * nc, ch), F32),
            pltpu.VMEM((n * np_, out), F32),
        ],
        name="compute",
    )(x, u, hx, hu, fc, fq)
    gradc, gradq, coef = pl.pallas_call(
        functools.partial(reduce_kernel, plan, n),
        out_shape=(sdt((pieces, nc, LANE), F32), sdt((pieces, rq, LANE), F32), sdt((2, 24, LANE), F32)),
        in_specs=[vmem] * 7,
        out_specs=(vmem,) * 3,
        scratch_shapes=both(half) + both(half) + both(2 * nm - 1, nz) + both(max(nz - 1, 1)) + both(nz)
        + [pltpu.VMEM((16, LANE), F32), pltpu.VMEM((n, 16, LANE), F32), pltpu.VMEM((8, LANE), F32)]
        + pair((n - 1,)) + pair((pieces, max(nz - 1, 1))) + pair((pieces, 2 * nm - 1))
        + pair((pieces, 2)) + pair((pieces + 1,)),
        compiler_params=pltpu.CompilerParams(collective_id=1, has_side_effects=True),
        name="reduce",
    )(pc, pq, wc, wp, stat, gc, gp)
    nwc, nwp, nmc, nmp = pl.pallas_call(
        functools.partial(update_kernel, plan),
        out_shape=(sdt((nc, ch), F32), sdt((np_, out), F32)) * 2,
        in_specs=[vmem] * 8,
        out_specs=(vmem,) * 4,
        name="update",
    )(gradc, gradq, coef, stat, wc, wp, mc_, mp)
    return (ig.reshape(block_input.shape), nwc.T, nmc.T, nwp.T, nmp.T)


def solution(mesh):
    in_specs = (
        P("batch", "rows", None, None),
        P("batch", "rows", None, None),
        P(None, "batch"),
        P(),
        P(None, "batch"),
        P(None, "batch"),
        P(),
        P(None, "batch"),
    )
    out_specs = (
        P("batch", "rows", None, None),
        P(None, "batch"),
        P(None, "batch"),
        P(None, "batch"),
        P(None, "batch"),
    )
    body = functools.partial(local, mesh.shape["batch"], mesh.shape["rows"])
    return jax.shard_map(body, mesh=mesh, in_specs=in_specs, out_specs=out_specs, check_vma=False)
```

```python
import functools
import math

import jax
import jax.numpy as jnp
from jax import lax
from jax.experimental import pallas as pl
from jax.experimental.pallas import tpu as pltpu
from jax.sharding import PartitionSpec as P

ws_eps = 0.0001
clip_ratio = 0.05
momentum_rate = 0.9
learn_rate = 1.6
norm_eps = 1e-06

F32 = jnp.float32
BF16 = jnp.bfloat16
MESH = pl.DeviceIdType.MESH
TAPS = 3
C0 = math.sqrt(2.0 / math.pi)
C1 = 0.044715


def gelu_parts(x):
    t = jnp.tanh(C0 * (x + C1 * (x * x * x)))
    half = 0.5 * (1.0 + t)
    slope = half + (0.5 * C0) * x * (1.0 - t * t) * (1.0 + (3.0 * C1) * (x * x))
    return x * half, slope


def dot_nn(a, b):
    return jnp.dot(a, b, preferred_element_type=F32)


def dot_nt(a, b):
    return lax.dot_general(a, b, (((1,), (1,)), ((), ())), preferred_element_type=F32)


def dot_tn(a, b):
    return lax.dot_general(a, b, (((0,), (0,)), ((), ())), preferred_element_type=F32)


LANE = 128


class Plan:
    def __init__(self, n, ch, out, nc, np_):
        nb = n.bit_length() - 1
        assert 2**nb == n and nb >= 1
        self.n, self.nc, self.np_ = n, nc, np_
        self.nz = 2 ** (nb // 2)
        self.nm = n // 2 // self.nz
        self.half = n // 2
        self.ch, self.out = ch, out
        self.nblk = out // ch
        self.pieces = ch // LANE
        cut = self.pieces // 2
        rest = self.pieces - cut
        self.sets = (
            [("q", k) for k in range(cut)] + [("c", k) for k in range(rest)],
            [("q", k) for k in range(cut, self.pieces)] + [("c", k) for k in range(rest, self.pieces)],
        )
        self.tiles = tuple([t for chunk in one for t in self.tiles_of(chunk)] for one in self.sets)
        self.wide = max(len(t) for t in self.tiles)
        assert self.wide <= 5
        self.proj_tiles = tuple(sum(which for which, _ in one) for one in self.tiles)

    def tiles_of(self, chunk):
        kind, k = chunk
        if kind == "c":
            return [(0, k * LANE)]
        return [(1, b * self.ch + k * LANE) for b in range(self.nblk)]

    def count_of(self, which):
        return self.np_ if which else self.nc

    def chunk_rows(self, kind):
        return self.nc if kind == "c" else self.nblk * self.np_

    def slot(self, d):
        return (d % 2 * self.nm + d // 2 % self.nm) * self.nz + d // 2 // self.nm

    def place(self, me):
        return me % 2, me // 2 % self.nm, me // 2 // self.nm

    def batch(self, c, m, z):
        return (z * self.nm + m) * 2 + c


def send(src, dst, sems, at, where):
    return pltpu.make_async_remote_copy(
        src_ref=src, dst_ref=dst, send_sem=sems[0].at[at], recv_sem=sems[1].at[at],
        device_id=where, device_id_type=MESH,
    )


def greet(plan):
    me = lax.axis_index("batch")
    r = lax.axis_index("rows")
    c, m, z = plan.place(me)
    n = plan.n
    barrier = pltpu.get_barrier_semaphore()
    for d in range(1, n):
        pl.semaphore_signal(barrier, inc=1, device_id={"batch": (me + d) % n}, device_id_type=MESH)
    for j in range(plan.nm):
        to = plan.batch(c, (m + j) % plan.nm, z)
        pl.semaphore_signal(barrier, inc=1, device_id={"batch": to, "rows": 1 - r}, device_id_type=MESH)


def greet_wait(plan):
    pl.semaphore_wait(pltpu.get_barrier_semaphore(), plan.n - 1 + plan.nm)


def push_all(plan, me, src, slots, sems):
    n = plan.n
    copies = []
    for d in range(1, n):
        copy = send(src, slots.at[me], sems, d - 1, {"batch": (me + d) % n})
        copy.start()
        copies.append(copy)
    slots[me] = src[...]
    return copies


def counts_of(plan, r):
    row = lax.broadcasted_iota(jnp.int32, (8, LANE), 0)
    first = jnp.where(r == 0, plan.proj_tiles[0], plan.proj_tiles[1])
    return jnp.where(row < first, float(plan.np_), float(plan.nc))


def merged(plan, slots, cnt):
    w = plan.wide
    total = slots[0]
    for i in range(1, plan.n):
        total = total + slots[i]
    mean = total[0:8] / (plan.n * cnt)
    between = None
    for i in range(plan.n):
        off = slots[i, 0:8] / cnt - mean
        term = cnt * (off * off)
        between = term if between is None else between + term
    return total, mean[0:w], total[w : 2 * w] + between[0:w]


def by_half(r, fn):
    for rr in range(2):
        @pl.when(r == rr)
        def _(rr=rr):
            fn(rr)


def shifted(vals, step, mc):
    rows = vals.shape[0]
    col = lax.broadcasted_iota(jnp.int32, vals.shape, 0)
    if step > 0:
        return jnp.where(col == mc - 1, 0.0, pltpu.roll(vals, rows - 1, 0))
    return jnp.where(col == 0, 0.0, pltpu.roll(vals, 1, 0))


class Refs:
    pass


def main_kernel(plan, names, mr, mc, gw, images, *refs):
    t = Refs()
    for name, ref in zip(names, refs, strict=True):
        setattr(t, name, ref)
    me = lax.axis_index("batch")
    r = lax.axis_index("rows")
    c, m, z = plan.place(me)
    n, nz, nm, w, half = plan.n, plan.nz, plan.nm, plan.wide, plan.half
    nc, np_, nblk, ch = plan.nc, plan.np_, plan.nblk, plan.ch
    groups = ch // gw
    wide = TAPS * gw
    px = mr * mc
    w_refs = (t.wc, t.wp)
    gain_refs = (t.gc, t.gp)
    full = {"c": t.fc, "q": t.fq}
    load_x = pltpu.make_async_copy(t.x_any, t.x, t.load.at[0])
    load_u = pltpu.make_async_copy(t.u_any, t.u, t.load.at[1])
    load_x.start()
    load_u.start()
    greet(plan)

    t.src[...] = jnp.zeros_like(t.src)

    def weight_stats(rr):
        for i, (which, col) in enumerate(plan.tiles[rr]):
            piece = w_refs[which][:, col : col + LANE]
            s = jnp.sum(piece, axis=0, keepdims=True)
            cent = piece - s / piece.shape[0]
            t.src[i : i + 1] = s
            t.src[w + i : w + i + 1] = jnp.sum(cent * cent, axis=0, keepdims=True)

    by_half(r, weight_stats)
    greet_wait(plan)
    push = push_all(plan, me, t.src, t.slots, (t.s_send, t.s_recv))
    halos = []
    for at, (load, ref, out) in enumerate(((load_x, t.x, t.hx), (load_u, t.u, t.hu))):
        load.wait()
        width = out.shape[0]
        first = (1 - r) * (ref.shape[0] - width)
        copy = send(ref.at[pl.ds(first, width)], out, (t.h_send, t.h_recv), at, {"rows": 1 - r})
        copy.start()
        halos.append(copy)

    def place(at, vals):
        act = gelu_parts(vals)[0].astype(BF16).astype(F32)
        for j in range(TAPS):
            moved = act if j == 1 else shifted(act, j - 1, mc)
            moved = moved.astype(BF16)
            for g in range(groups):
                t.xs[pl.ds(at, mc), g * wide + j * gw : g * wide + (j + 1) * gw] = moved[
                    :, g * gw : (g + 1) * gw
                ]

    def body(row, carry):
        at = pl.multiple_of(row * mc, mc)
        place(pl.multiple_of(at + 2 * mc, mc), t.x[pl.ds(at, mc)].astype(F32))
        return carry

    lax.fori_loop(0, mr, body, 0)

    for copy in push:
        copy.wait()
    cnt = counts_of(plan, r)
    _, mean, spread = merged(plan, t.slots, cnt)
    t.stat[r] = jnp.zeros_like(t.stat[0])
    t.stat[r, 0:w] = mean
    t.stat[r, 8 : 8 + w] = spread
    copy = send(t.stat.at[r], t.stat.at[r], (t.h_send, t.h_recv), 2, {"rows": 1 - r})
    copy.start()
    halos.append(copy)
    factor = lax.rsqrt(spread + ws_eps)
    slot = (c * nm + m) * nz + z
    base = (c * nm + m) * nz

    def z_copy(k, j, chunk):
        kind, g = chunk
        at = full[kind].at[g, slot]
        return send(at, at, (t.z_send, t.z_recv), (k, j - 1), {"batch": plan.batch(c, m, (z + j) % nz)})

    def start_z(rr):
        i = 0
        for k, chunk in enumerate(plan.sets[rr]):
            kind, g = chunk
            for b, (which, col) in enumerate(plan.tiles_of(chunk)):
                count = plan.count_of(which)
                scale = gain_refs[which][col : col + LANE][None] * factor[i : i + 1]
                std = (scale * (w_refs[which][:, col : col + LANE] - mean[i : i + 1])).astype(BF16)
                full[kind][g, slot, b * count : (b + 1) * count] = std
                i += 1
            for j in range(1, nz):
                z_copy(k, j, chunk).start()

    by_half(r, start_z)

    def m_copy(k, j, jx, chunk):
        kind, g = chunk
        at = full[kind].at[g, pl.ds(base, nz)]
        where = {"batch": plan.batch(c, (m + j) % nm, z), "rows": (r + jx) % 2}
        return send(at, at, (t.m_send, t.m_recv), (k, jx * nm + j - 1), where)

    peers = [(j, jx) for jx in (1, 0) for j in reversed(range(nm)) if (j, jx) != (0, 0)]

    def spread_m(k):
        def fn(rr):
            chunk = plan.sets[rr][k]
            for j in range(1, nz):
                z_copy(k, j, chunk).wait()
            for j, jx in peers:
                m_copy(k, j, jx, chunk).start()
        by_half(r, fn)

    def finish_m(k):
        def fn(rr):
            for j, jx in peers:
                m_copy(k, j, jx, plan.sets[rr][k]).wait_send()
                m_copy(k, j, jx, plan.sets[(rr + jx) % 2][k]).wait_recv()
        by_half(r, fn)
        for side in range(2):
            d_copy(k, side).start()

    def d_copy(k, side):
        kind, g = plan.sets[side][k]
        at = full[kind].at[g, pl.ds(c * half, half)]
        return send(at, at, (t.d_send, t.d_recv), (k, side), {"batch": plan.batch(1 - c, m, z)})

    def unpack(chunk):
        kind, g = chunk
        lanes = slice(g * LANE, (g + 1) * LANE)
        for d in range(n):
            if kind == "c":
                t.kt[d * nc : (d + 1) * nc, lanes] = t.fc[g, plan.slot(d)]
                continue
            for b in range(nblk):
                t.pt[d * np_ : (d + 1) * np_, b * ch + g * LANE : b * ch + (g + 1) * LANE] = t.fq[
                    g, plan.slot(d), b * np_ : (b + 1) * np_
                ]

    def forward(g, e, up):
        rows = up.shape[0]
        hg = dot_nt(up, t.pt[g * gw : (g + 1) * gw])
        acc = None
        for i in range(TAPS):
            term = dot_nn(
                t.xs[pl.ds(pl.multiple_of((e + i) * mc, mc), rows), g * wide : (g + 1) * wide],
                t.kt[i * wide : (i + 1) * wide, g * gw : (g + 1) * gw],
            )
            acc = term if acc is None else acc + term
        h, slope = gelu_parts(acc)
        t.hid[pl.ds(pl.multiple_of(e * mc, mc), rows), g * gw : (g + 1) * gw] = h.astype(BF16)
        grad = (hg * slope).astype(BF16).astype(F32)
        for q in range(rows // mc):
            here = grad[q * mc : (q + 1) * mc]
            for j in range(TAPS):
                moved = here if j == 1 else shifted(here, 1 - j, mc)
                t.ys[pl.ds(pl.multiple_of((e + q) * mc, mc), mc), g * wide + j * gw : g * wide + (j + 1) * gw] = moved.astype(BF16)

    many = next(k for k in (4, 2, 1) if mr % k == 0)

    def forward_all(g):
        forward(g, jnp.where(r == 1, 0, mr + 1), t.hu[...])

        def fwd(s, carry):
            up = t.u[pl.ds(pl.multiple_of(s * many * mc, mc), many * mc)]
            forward(g, 1 + s * many, up)
            return carry

        lax.fori_loop(0, mr // many, fwd, 0)

    halos[0].wait()
    near = pl.multiple_of(jnp.where(r == 1, 0, (mr + 2) * mc), mc)
    far = pl.multiple_of(jnp.where(r == 1, (mr + 2) * mc, 0), mc)
    t.xs[pl.ds(far, 2 * mc)] = jnp.zeros((2 * mc, t.xs.shape[1]), BF16)
    for e in range(2):
        place(pl.multiple_of(near + e * mc, mc), t.hx[e * mc : (e + 1) * mc].astype(F32))
    outside = pl.multiple_of(jnp.where(r == 1, (mr + 1) * mc, 0), mc)
    t.ys[pl.ds(outside, mc)] = jnp.zeros((mc, t.ys.shape[1]), BF16)
    halos[1].wait()

    for k in range(plan.pieces):
        spread_m(k)
    filled, ran = [], []
    for k in range(plan.pieces):
        finish_m(k)
        if k == 0:
            continue
        upto = k + 1 if k == plan.pieces - 1 else k
        for q in range(k - 1, upto):
            for side in range(2):
                d_copy(q, side).wait()
                unpack(plan.sets[side][q])
                filled.append(plan.sets[side][q])
            if sum(kind == "q" for kind, _ in filled) == plan.pieces:
                for kind, g in filled:
                    if kind == "c" and g not in ran:
                        forward_all(g)
                        ran.append(g)
    assert len(ran) == groups

    part = {"c": t.pc, "q": t.pq}
    got_d = {"c": t.gdc, "q": t.gdq}
    two = {"c": t.twoc, "q": t.twoq}
    got_m = {"c": t.gmc, "q": t.gmq}
    eight = {"c": t.eightc, "q": t.eightq}
    got_z = {"c": t.gzc, "q": t.gzq}
    grads = {"c": t.gradc, "q": t.gradq}

    def produce(chunk):
        kind, g = chunk
        if kind == "c":
            own = t.ys[mc : mc + px, g * wide + gw : g * wide + 2 * gw]
            for i in range(TAPS):
                t.cg[i * wide : (i + 1) * wide] = dot_tn(
                    t.xs[(1 + i) * mc : (1 + i) * mc + px, g * wide : (g + 1) * wide], own
                )
            for d in range(n):
                t.pc[g, plan.slot(d)] = t.cg[d * nc : (d + 1) * nc].astype(BF16)
            return
        for b in range(nblk):
            at = b * ch + g * LANE
            t.pg[:, b * LANE : (b + 1) * LANE] = dot_tn(t.hid[mc : mc + px], t.u[:, at : at + LANE])
        for d in range(n):
            for b in range(nblk):
                t.pq[g, plan.slot(d), b * np_ : (b + 1) * np_] = t.pg[
                    d * np_ : (d + 1) * np_, b * LANE : (b + 1) * LANE
                ].astype(BF16)

    def rd_copy(k, side):
        kind, g = plan.sets[side][k]
        return send(
            part[kind].at[g, pl.ds((1 - c) * half, half)], got_d[kind].at[g],
            (t.rd_send, t.rd_recv), (k, side), {"batch": plan.batch(1 - c, m, z)},
        )

    def rm_copy(k, j, jx, chunk):
        kind, g = chunk
        to = (m + j) % nm
        return send(
            two[kind].at[g, pl.ds(to * nz, nz)], got_m[kind].at[g, jx * nm + j - 1],
            (t.rm_send, t.rm_recv), (k, jx * nm + j - 1),
            {"batch": plan.batch(c, to, z), "rows": (r + jx) % 2},
        )

    def step_m(k):
        for side in range(2):
            rd_copy(k, side).wait()

        def fn(rr):
            for j, jx in peers:
                kind, g = plan.sets[(rr + jx) % 2][k]
                first = (m + j) % nm * nz
                two[kind][g, pl.ds(first, nz)] = (
                    part[kind][g, pl.ds(c * half + first, nz)] + got_d[kind][g, pl.ds(first, nz)]
                )
                rm_copy(k, j, jx, (kind, g)).start()
        by_half(r, fn)

    def rz_copy(k, j, chunk):
        kind, g = chunk
        to = (z + j) % nz
        return send(
            eight[kind].at[g, to], got_z[kind].at[g, j - 1],
            (t.rz_send, t.rz_recv), (k, j - 1), {"batch": plan.batch(c, m, to)},
        )

    def sum_m(kind, g, at):
        first = m * nz + at
        total = part[kind][g, c * half + first].astype(F32) + got_d[kind][g, first].astype(F32)
        for i in range(2 * nm - 1):
            total = total + got_m[kind][g, i, at].astype(F32)
        return total

    def step_z(k):
        def fn(rr):
            for j, jx in peers:
                rm_copy(k, j, jx, plan.sets[(rr + jx) % 2][k]).wait_send()
                rm_copy(k, j, jx, plan.sets[rr][k]).wait_recv()
            kind, g = plan.sets[rr][k]
            for j in range(1, nz):
                to = (z + j) % nz
                eight[kind][g, to] = sum_m(kind, g, to).astype(BF16)
                rz_copy(k, j, (kind, g)).start()
            grads[kind][g] = sum_m(kind, g, z)
        by_half(r, fn)

    def x_copy(k, chunk):
        kind, g = chunk
        return send(grads[kind].at[g], grads[kind].at[g], (t.x_send, t.x_recv), k, {"rows": 1 - r})

    def finish(k):
        def fn(rr):
            kind, g = plan.sets[rr][k]
            total = grads[kind][g]
            for j in range(1, nz):
                rz_copy(k, j, (kind, g)).wait()
                total = total + got_z[kind][g, j - 1].astype(F32)
            grads[kind][g] = total / images
            x_copy(k, (kind, g)).start()
        by_half(r, fn)

    order = list(reversed(range(plan.pieces)))
    before = None
    for k in order:
        for side in range(2):
            produce(plan.sets[side][k])
            rd_copy(k, side).start()
        if before is not None:
            step_m(before)
        before = k
    step_m(before)

    tall = next(k for k in (2, 1) if mr % k == 0)

    def back(s, carry):
        at = pl.multiple_of(s * tall * mc, mc)
        for g in range(groups):
            acc = None
            for i in range(TAPS):
                for j in range(TAPS):
                    term = dot_nt(
                        t.ys[pl.ds(pl.multiple_of(at + (2 - i) * mc, mc), tall * mc), g * wide + j * gw : g * wide + (j + 1) * gw],
                        t.kt[i * wide + j * gw : i * wide + (j + 1) * gw, g * gw : (g + 1) * gw],
                    )
                    acc = term if acc is None else acc + term
            slope = gelu_parts(t.x[pl.ds(at, tall * mc), g * gw : (g + 1) * gw].astype(F32))[1]
            t.ig[pl.ds(at, tall * mc), g * gw : (g + 1) * gw] = (acc * slope).astype(BF16)
        return carry

    lax.fori_loop(0, mr // tall, back, 0)
    store = pltpu.make_async_copy(t.ig, t.ig_any, t.load.at[2])
    store.start()
    for k in order:
        step_z(k)
    for k in order:
        finish(k)

    t.src[...] = jnp.zeros_like(t.src)
    t.gain[...] = jnp.zeros_like(t.gain)

    def grad_stats(rr):
        i = 0
        for chunk in plan.sets[rr]:
            kind, g = chunk
            for b, (which, col) in enumerate(plan.tiles_of(chunk)):
                count = plan.count_of(which)
                piece = grads[kind][g, b * count : (b + 1) * count]
                cent = w_refs[which][:, col : col + LANE] - t.stat[rr, i : i + 1]
                s = jnp.sum(piece, axis=0, keepdims=True)
                off = piece - s / count
                t.src[i : i + 1] = s
                t.src[w + i : w + i + 1] = jnp.sum(off * off, axis=0, keepdims=True)
                t.src[2 * w + i : 2 * w + i + 1] = jnp.sum(piece * cent, axis=0, keepdims=True)
                t.gain[i : i + 1] = gain_refs[which][col : col + LANE][None]
                i += 1

    by_half(r, grad_stats)
    for copy in push_all(plan, me, t.src, t.slots2, (t.s2_send, t.s2_recv)):
        copy.wait()
    total, gmean, gspread = merged(plan, t.slots2, cnt)
    proj = total[2 * w : 3 * w]
    fan = n * cnt[0:w]
    mean = t.stat[r, 0:w]
    spread = t.stat[r, 8 : 8 + w]
    factor = lax.rsqrt(spread + ws_eps)
    f2 = factor * factor
    one = t.gain[0:w] * factor
    coef_two = one * f2 * proj
    grad_sq = one * one * jnp.maximum(gspread - f2 * proj * proj * (2.0 - f2 * spread), 0.0)
    weight_sq = spread + fan * (mean * mean)
    clip = jnp.minimum(1.0, clip_ratio * jnp.sqrt(weight_sq) * lax.rsqrt(grad_sq + norm_eps))
    t.coef[r] = jnp.zeros_like(t.coef[0])
    t.coef[r, 0:w] = clip * one
    t.coef[r, 8 : 8 + w] = gmean
    t.coef[r, 16 : 16 + w] = clip * coef_two
    last = send(t.coef.at[r], t.coef.at[r], (t.x_send, t.x_recv), plan.pieces, {"rows": 1 - r})
    last.start()

    def end(rr):
        for k in range(plan.pieces):
            x_copy(k, plan.sets[rr][k]).wait_send()
            x_copy(k, plan.sets[1 - rr][k]).wait_recv()

    by_half(r, end)
    halos[2].wait()
    store.wait()
    last.wait()


def update_kernel(plan, gradc_ref, gradq_ref, coef_ref, stat_ref, wc_ref, wp_ref, mc_ref, mp_ref, ig_in,
                  nwc_ref, nwp_ref, nmc_ref, nmp_ref, ig_out, ig, sems):
    fetch = pltpu.make_async_copy(ig_in, ig, sems.at[0])
    store = pltpu.make_async_copy(ig, ig_out, sems.at[1])
    fetch.start()
    fetch.wait()
    store.start()
    grads = {"c": gradc_ref, "q": gradq_ref}
    for rr in range(2):
        i = 0
        for chunk in plan.sets[rr]:
            kind, g = chunk
            for b, (which, col) in enumerate(plan.tiles_of(chunk)):
                count = plan.count_of(which)
                cols = slice(col, col + LANE)
                w = (wc_ref, wp_ref)[which][:, cols]
                grad = grads[kind][g, b * count : (b + 1) * count]
                clipped = coef_ref[rr, i : i + 1] * (grad - coef_ref[rr, 8 + i : 9 + i]) - coef_ref[
                    rr, 16 + i : 17 + i
                ] * (w - stat_ref[rr, i : i + 1])
                new_m = momentum_rate * (mc_ref, mp_ref)[which][:, cols] + clipped
                (nmc_ref, nmp_ref)[which][:, cols] = new_m
                (nwc_ref, nwp_ref)[which][:, cols] = w - learn_rate * (clipped + momentum_rate * new_m)
                i += 1
    store.wait()


def local(n, nrows, block_input, output_grad, conv_weight, conv_gain, conv_momentum,
          proj_weight, proj_gain, proj_momentum):
    assert nrows == 2
    _, mr, mc, ch = block_input.shape
    out = output_grad.shape[3]
    nc = conv_weight.shape[1]
    np_ = proj_weight.shape[1]
    gw = nc * n // (TAPS * TAPS)
    assert gw == LANE
    plan = Plan(n, ch, out, nc, np_)
    nz, nm, half, pieces = plan.nz, plan.nm, plan.half, plan.pieces
    px = mr * mc
    rq = plan.chunk_rows("q")

    wc, wp, mc_, mp = conv_weight.T, proj_weight.T, conv_momentum.T, proj_momentum.T
    gc, gp = conv_gain, proj_gain
    x = block_input.reshape(px, ch)
    u = output_grad.reshape(px, out)
    vmem = pl.BlockSpec(memory_space=pltpu.VMEM)
    anym = pl.BlockSpec(memory_space=pl.ANY)
    sdt = jax.ShapeDtypeStruct
    dma = pltpu.SemaphoreType.DMA
    scratch = {}

    def pair(name, shape):
        scratch[name + "_send"] = dma(shape)
        scratch[name + "_recv"] = dma(shape)

    def both(name, *lead):
        scratch[name + "c"] = pltpu.VMEM((pieces, *lead, nc, LANE), BF16)
        scratch[name + "q"] = pltpu.VMEM((pieces, *lead, rq, LANE), BF16)

    scratch.update(
        x=pltpu.VMEM((px, ch), BF16),
        u=pltpu.VMEM((px, out), BF16),
        ig=pltpu.VMEM((px, ch), BF16),
        hx=pltpu.VMEM((2 * mc, ch), BF16),
        hu=pltpu.VMEM((mc, out), BF16),
        kt=pltpu.VMEM((n * nc, ch), BF16),
        pt=pltpu.VMEM((n * np_, out), BF16),
        xs=pltpu.VMEM(((mr + 4) * mc, TAPS * ch), BF16),
        ys=pltpu.VMEM(((mr + 2) * mc, TAPS * ch), BF16),
        hid=pltpu.VMEM(((mr + 2) * mc, ch), BF16),
        cg=pltpu.VMEM((n * nc, LANE), F32),
        pg=pltpu.VMEM((n * np_, plan.nblk * LANE), F32),
        src=pltpu.VMEM((16, LANE), F32),
        slots=pltpu.VMEM((n, 16, LANE), F32),
        slots2=pltpu.VMEM((n, 16, LANE), F32),
        gain=pltpu.VMEM((8, LANE), F32),
        load=dma((3,)),
    )
    for name, lead in (("f", (n,)), ("p", (n,)), ("gd", (half,)), ("two", (half,)),
                       ("gm", (2 * nm - 1, nz)), ("eight", (nz,)), ("gz", (max(nz - 1, 1),))):
        both(name, *lead)
    for name in ("s", "s2"):
        pair(name, (n - 1,))
    for name in ("z", "rz"):
        pair(name, (pieces, max(nz - 1, 1)))
    for name in ("m", "rm"):
        pair(name, (pieces, 2 * nm - 1))
    for name in ("d", "rd"):
        pair(name, (pieces, 2))
    pair("h", (3,))
    pair("x", (pieces + 1,))
    names = ["wc", "wp", "gc", "gp", "x_any", "u_any", "ig_any", "gradc", "gradq", "coef", "stat", *scratch]
    ig, gradc, gradq, coef, stat = pl.pallas_call(
        functools.partial(main_kernel, plan, names, mr, mc, gw, n),
        out_shape=(
            sdt((px, ch), BF16),
            sdt((pieces, nc, LANE), F32),
            sdt((pieces, rq, LANE), F32),
            sdt((2, 24, LANE), F32),
            sdt((2, 16, LANE), F32),
        ),
        in_specs=[vmem] * 4 + [anym] * 2,
        out_specs=(anym,) + (vmem,) * 4,
        scratch_shapes=list(scratch.values()),
        compiler_params=pltpu.CompilerParams(collective_id=0, has_side_effects=True),
        name="main",
    )(wc, wp, gc, gp, x, u)
    nwc, nwp, nmc, nmp, ig = pl.pallas_call(
        functools.partial(update_kernel, plan),
        out_shape=(sdt((nc, ch), F32), sdt((np_, out), F32)) * 2 + (sdt((px, ch), BF16),),
        in_specs=[vmem] * 8 + [anym],
        out_specs=(vmem,) * 4 + (anym,),
        scratch_shapes=[pltpu.VMEM((px, ch), BF16), dma((2,))],
        name="update",
    )(gradc, gradq, coef, stat, wc, wp, mc_, mp, ig)
    return (ig.reshape(block_input.shape), nwc.T, nmc.T, nwp.T, nmp.T)


def solution(mesh):
    in_specs = (
        P("batch", "rows", None, None),
        P("batch", "rows", None, None),
        P(None, "batch"),
        P(),
        P(None, "batch"),
        P(None, "batch"),
        P(),
        P(None, "batch"),
    )
    out_specs = (
        P("batch", "rows", None, None),
        P(None, "batch"),
        P(None, "batch"),
        P(None, "batch"),
        P(None, "batch"),
    )
    body = functools.partial(local, mesh.shape["batch"], mesh.shape["rows"])
    return jax.shard_map(body, mesh=mesh, in_specs=in_specs, out_specs=out_specs, check_vma=False)
```

```python
import functools
import math

import jax
import jax.numpy as jnp
from jax import lax
from jax.experimental import pallas as pl
from jax.experimental.pallas import tpu as pltpu
from jax.sharding import PartitionSpec as P

ws_eps = 0.0001
clip_ratio = 0.05
momentum_rate = 0.9
learn_rate = 1.6
norm_eps = 1e-06

F32 = jnp.float32
BF16 = jnp.bfloat16
MESH = pl.DeviceIdType.MESH
TAPS = 3
C0 = math.sqrt(2.0 / math.pi)
C1 = 0.044715


def gelu_parts(x):
    t = jnp.tanh(C0 * (x + C1 * (x * x * x)))
    half = 0.5 * (1.0 + t)
    slope = half + (0.5 * C0) * x * (1.0 - t * t) * (1.0 + (3.0 * C1) * (x * x))
    return x * half, slope


def dot_nn(a, b):
    return jnp.dot(a, b, preferred_element_type=F32)


def dot_nt(a, b):
    return lax.dot_general(a, b, (((1,), (1,)), ((), ())), preferred_element_type=F32)


def dot_tn(a, b):
    return lax.dot_general(a, b, (((0,), (0,)), ((), ())), preferred_element_type=F32)


LANE = 128


class Plan:
    def __init__(self, n, ch, out, nc, np_):
        nb = n.bit_length() - 1
        assert 2**nb == n and nb >= 1
        self.n, self.nc, self.np_ = n, nc, np_
        self.nz = 2 ** (nb // 2)
        self.nm = n // 2 // self.nz
        self.half = n // 2
        self.ch, self.out = ch, out
        self.nblk = out // ch
        self.pieces = ch // LANE
        cut = self.pieces // 2
        rest = self.pieces - cut
        self.sets = (
            [("q", k) for k in range(cut)] + [("c", k) for k in range(rest)],
            [("q", k) for k in range(cut, self.pieces)] + [("c", k) for k in range(rest, self.pieces)],
        )
        self.tiles = tuple([t for chunk in one for t in self.tiles_of(chunk)] for one in self.sets)
        self.lead = self.nblk
        self.wide = max(len(t) for t in self.tiles)
        assert cut and self.wide <= 8 and self.wide - self.lead <= 4
        self.starts = tuple(
            [sum(len(self.tiles_of(chunk)) for chunk in one[:k]) for k in range(self.pieces)] for one in self.sets
        )

    def tiles_of(self, chunk):
        kind, k = chunk
        if kind == "c":
            return [(0, k * LANE)]
        return [(1, b * self.ch + k * LANE) for b in range(self.nblk)]

    def count_of(self, which):
        return self.np_ if which else self.nc

    def chunk_rows(self, kind):
        return self.nc if kind == "c" else self.nblk * self.np_

    def slot(self, d):
        return (d % 2 * self.nm + d // 2 % self.nm) * self.nz + d // 2 // self.nm

    def place(self, me):
        return me % 2, me // 2 % self.nm, me // 2 // self.nm

    def batch(self, c, m, z):
        return (z * self.nm + m) * 2 + c


def send(src, dst, sems, at, where):
    return pltpu.make_async_remote_copy(
        src_ref=src, dst_ref=dst, send_sem=sems[0].at[at], recv_sem=sems[1].at[at],
        device_id=where, device_id_type=MESH,
    )


def greet(plan):
    me = lax.axis_index("batch")
    r = lax.axis_index("rows")
    n = plan.n
    barrier = pltpu.get_barrier_semaphore()
    for d in range(1, n):
        pl.semaphore_signal(barrier, inc=1, device_id={"batch": (me + d) % n}, device_id_type=MESH)
    for d in range(plan.half):
        to = (me + 2 * d) % n
        pl.semaphore_signal(barrier, inc=1, device_id={"batch": to, "rows": 1 - r}, device_id_type=MESH)


def greet_wait(plan):
    pl.semaphore_wait(pltpu.get_barrier_semaphore(), plan.n - 1 + plan.half)


def merged(entries, cnt):
    total = entries[0]
    for one in entries[1:]:
        total = total + one
    mean = total / (len(entries) * cnt)
    between = None
    for one in entries:
        off = one / cnt - mean
        term = cnt * (off * off)
        between = term if between is None else between + term
    return total, mean, between


def by_half(r, fn):
    for rr in range(2):
        @pl.when(r == rr)
        def _(rr=rr):
            fn(rr)


def shifted(vals, step, mc):
    rows = vals.shape[0]
    col = lax.broadcasted_iota(jnp.int32, vals.shape, 0)
    if step > 0:
        return jnp.where(col == mc - 1, 0.0, pltpu.roll(vals, rows - 1, 0))
    return jnp.where(col == 0, 0.0, pltpu.roll(vals, 1, 0))


class Refs:
    pass


def main_kernel(plan, names, mr, mc, gw, images, *refs):
    t = Refs()
    for name, ref in zip(names, refs, strict=True):
        setattr(t, name, ref)
    me = lax.axis_index("batch")
    r = lax.axis_index("rows")
    c, m, z = plan.place(me)
    n, nz, nm, half = plan.n, plan.nz, plan.nm, plan.half
    nc, np_, nblk, ch = plan.nc, plan.np_, plan.nblk, plan.ch
    groups = ch // gw
    wide = TAPS * gw
    px = mr * mc
    w_refs = (t.wc, t.wp)
    gain_refs = (t.gc, t.gp)
    full = {"c": t.fc, "q": t.fq}
    loads = []
    for at, (far, near) in enumerate(((t.wc_any, t.wc), (t.wp_any, t.wp), (t.gc_any, t.gc), (t.gp_any, t.gp),
                                      (t.x_any, t.x), (t.u_any, t.u))):
        copy = pltpu.make_async_copy(far, near, t.load.at[at])
        copy.start()
        loads.append(copy)
    greet(plan)

    t.src[...] = jnp.zeros_like(t.src)

    def weight_stats(rr):
        for i, (which, col) in enumerate(plan.tiles[rr]):
            piece = w_refs[which][:, col : col + LANE]
            s = jnp.sum(piece, axis=0, keepdims=True)
            cent = piece - s / piece.shape[0]
            late = int(i >= plan.lead)
            row = i - late * plan.lead
            t.src[late, row : row + 1] = s
            t.src[late, 4 + row : 5 + row] = jnp.sum(cent * cent, axis=0, keepdims=True)

    for copy in loads[:4]:
        copy.wait()
    by_half(r, weight_stats)
    greet_wait(plan)
    push = [[], []]
    for late in range(2):
        for d in range(1, n):
            copy = send(
                t.src.at[late], t.slots.at[late, me], (t.s_send, t.s_recv), (late, d - 1), {"batch": (me + d) % n}
            )
            copy.start()
            push[late].append(copy)
        t.slots[late, me] = t.src[late]
    halos = []
    for at, (load, ref, out) in enumerate(((loads[4], t.x, t.hx), (loads[5], t.u, t.hu))):
        load.wait()
        width = out.shape[0]
        first = (1 - r) * (ref.shape[0] - width)
        copy = send(ref.at[pl.ds(first, width)], out, (t.h_send, t.h_recv), at, {"rows": 1 - r})
        copy.start()
        halos.append(copy)

    def place(at, vals):
        act = gelu_parts(vals)[0].astype(BF16).astype(F32)
        for j in range(TAPS):
            moved = act if j == 1 else shifted(act, j - 1, mc)
            moved = moved.astype(BF16)
            for g in range(groups):
                t.xs[pl.ds(at, mc), g * wide + j * gw : g * wide + (j + 1) * gw] = moved[
                    :, g * gw : (g + 1) * gw
                ]

    def body(row, carry):
        at = pl.multiple_of(row * mc, mc)
        place(pl.multiple_of(at + 2 * mc, mc), t.x[pl.ds(at, mc)].astype(F32))
        return carry

    lax.fori_loop(0, mr, body, 0)
    t.gain[...] = jnp.zeros_like(t.gain)
    for rr in range(2):
        for i, (which, col) in enumerate(plan.tiles[rr]):
            t.gain[rr, i : i + 1] = gain_refs[which][col : col + LANE][None]

    slot = (c * nm + m) * nz + z
    base = (c * nm + m) * nz

    def z_copy(k, j, chunk):
        kind, g = chunk
        at = full[kind].at[g, slot]
        return send(at, at, (t.z_send, t.z_recv), (k, j - 1), {"batch": plan.batch(c, m, (z + j) % nz)})

    t.stat[r] = jnp.zeros_like(t.stat[0])
    row = lax.broadcasted_iota(jnp.int32, (8, LANE), 0)
    for late in range(2):
        for copy in push[late]:
            copy.wait()
        ks = range(1, plan.pieces) if late else range(1)
        tiles = [plan.tiles[rr][plan.lead :] if late else plan.tiles[rr][: plan.lead] for rr in range(2)]
        first = [sum(which for which, _ in one) for one in tiles]
        most = max(len(one) for one in tiles)
        cnt = jnp.where(row < jnp.where(r == 0, first[0], first[1]), float(np_), float(nc))
        total, mean, between = merged([t.slots[late, i] for i in range(n)], cnt)
        spread = total[4 : 4 + most] + between[0:most]
        factor = lax.rsqrt(spread + ws_eps)
        at = late * plan.lead
        t.stat[r, at : at + most] = mean[0:most]
        t.stat[r, 8 + at : 8 + at + most] = spread

        def start_z(rr, ks=ks, mean=mean, factor=factor):
            i = 0
            for k in ks:
                kind, g = plan.sets[rr][k]
                for b, (which, col) in enumerate(plan.tiles_of((kind, g))):
                    count = plan.count_of(which)
                    scale = gain_refs[which][col : col + LANE][None] * factor[i : i + 1]
                    std = (scale * (w_refs[which][:, col : col + LANE] - mean[i : i + 1])).astype(BF16)
                    full[kind][g, slot, b * count : (b + 1) * count] = std
                    i += 1
                for j in range(1, nz):
                    z_copy(k, j, (kind, g)).start()

        by_half(r, start_z)
    copy = send(t.stat.at[r], t.stat.at[r], (t.h_send, t.h_recv), 2, {"rows": 1 - r})
    copy.start()
    halos.append(copy)

    def m_copy(k, j, jx, chunk):
        kind, g = chunk
        at = full[kind].at[g, pl.ds(base, nz)]
        where = {"batch": plan.batch(c, (m + j) % nm, z), "rows": (r + jx) % 2}
        return send(at, at, (t.m_send, t.m_recv), (k, jx * nm + j - 1), where)

    peers = [(j, jx) for jx in (1, 0) for j in reversed(range(nm)) if (j, jx) != (0, 0)]

    def spread_m(k):
        def fn(rr):
            chunk = plan.sets[rr][k]
            for j in range(1, nz):
                z_copy(k, j, chunk).wait()
            for j, jx in peers:
                m_copy(k, j, jx, chunk).start()
        by_half(r, fn)

    def finish_m(k):
        def fn(rr):
            for j, jx in peers:
                m_copy(k, j, jx, plan.sets[rr][k]).wait_send()
                m_copy(k, j, jx, plan.sets[(rr + jx) % 2][k]).wait_recv()
        by_half(r, fn)
        for side in range(2):
            d_copy(k, side).start()

    def d_copy(k, side):
        kind, g = plan.sets[side][k]
        at = full[kind].at[g, pl.ds(c * half, half)]
        return send(at, at, (t.d_send, t.d_recv), (k, side), {"batch": plan.batch(1 - c, m, z)})

    def unpack(chunk):
        kind, g = chunk
        lanes = slice(g * LANE, (g + 1) * LANE)
        for d in range(n):
            if kind == "c":
                t.kt[d * nc : (d + 1) * nc, lanes] = t.fc[g, plan.slot(d)]
                continue
            for b in range(nblk):
                t.pt[d * np_ : (d + 1) * np_, b * ch + g * LANE : b * ch + (g + 1) * LANE] = t.fq[
                    g, plan.slot(d), b * np_ : (b + 1) * np_
                ]

    def forward(g, e, up):
        rows = up.shape[0]
        hg = dot_nt(up, t.pt[g * gw : (g + 1) * gw])
        acc = None
        for i in range(TAPS):
            term = dot_nn(
                t.xs[pl.ds(pl.multiple_of((e + i) * mc, mc), rows), g * wide : (g + 1) * wide],
                t.kt[i * wide : (i + 1) * wide, g * gw : (g + 1) * gw],
            )
            acc = term if acc is None else acc + term
        h, slope = gelu_parts(acc)
        t.hid[pl.ds(pl.multiple_of(e * mc, mc), rows), g * gw : (g + 1) * gw] = h.astype(BF16)
        grad = (hg * slope).astype(BF16).astype(F32)
        for q in range(rows // mc):
            here = grad[q * mc : (q + 1) * mc]
            for j in range(TAPS):
                moved = here if j == 1 else shifted(here, 1 - j, mc)
                t.ys[pl.ds(pl.multiple_of((e + q) * mc, mc), mc), g * wide + j * gw : g * wide + (j + 1) * gw] = moved.astype(BF16)

    many = next(k for k in (4, 2, 1) if mr % k == 0)

    def forward_all(g):
        forward(g, jnp.where(r == 1, 0, mr + 1), t.hu[...])

        def fwd(s, carry):
            up = t.u[pl.ds(pl.multiple_of(s * many * mc, mc), many * mc)]
            forward(g, 1 + s * many, up)
            return carry

        lax.fori_loop(0, mr // many, fwd, 0)

    halos[0].wait()
    near = pl.multiple_of(jnp.where(r == 1, 0, (mr + 2) * mc), mc)
    far = pl.multiple_of(jnp.where(r == 1, (mr + 2) * mc, 0), mc)
    t.xs[pl.ds(far, 2 * mc)] = jnp.zeros((2 * mc, t.xs.shape[1]), BF16)
    for e in range(2):
        place(pl.multiple_of(near + e * mc, mc), t.hx[e * mc : (e + 1) * mc].astype(F32))
    outside = pl.multiple_of(jnp.where(r == 1, (mr + 1) * mc, 0), mc)
    t.ys[pl.ds(outside, mc)] = jnp.zeros((mc, t.ys.shape[1]), BF16)
    halos[1].wait()

    for k in range(plan.pieces):
        spread_m(k)
    filled, ran = [], []
    for k in range(plan.pieces):
        finish_m(k)
        if k == 0:
            continue
        upto = k + 1 if k == plan.pieces - 1 else k
        for q in range(k - 1, upto):
            for side in range(2):
                d_copy(q, side).wait()
                unpack(plan.sets[side][q])
                filled.append(plan.sets[side][q])
            if sum(kind == "q" for kind, _ in filled) == plan.pieces:
                for kind, g in filled:
                    if kind == "c" and g not in ran:
                        forward_all(g)
                        ran.append(g)
    assert len(ran) == groups

    part = {"c": t.pc, "q": t.pq}
    got_d = {"c": t.gdc, "q": t.gdq}
    two = {"c": t.twoc, "q": t.twoq}
    got_m = {"c": t.gmc, "q": t.gmq}
    eight = {"c": t.eightc, "q": t.eightq}
    got_z = {"c": t.gzc, "q": t.gzq}
    grads = {"c": t.gradc, "q": t.gradq}

    def produce(chunk):
        kind, g = chunk
        if kind == "c":
            own = t.ys[mc : mc + px, g * wide + gw : g * wide + 2 * gw]
            for i in range(TAPS):
                t.cg[i * wide : (i + 1) * wide] = dot_tn(
                    t.xs[(1 + i) * mc : (1 + i) * mc + px, g * wide : (g + 1) * wide], own
                )
            for d in range(n):
                t.pc[g, plan.slot(d)] = t.cg[d * nc : (d + 1) * nc].astype(BF16)
            return
        for b in range(nblk):
            at = b * ch + g * LANE
            t.pg[:, b * LANE : (b + 1) * LANE] = dot_tn(t.hid[mc : mc + px], t.u[:, at : at + LANE])
        for d in range(n):
            for b in range(nblk):
                t.pq[g, plan.slot(d), b * np_ : (b + 1) * np_] = t.pg[
                    d * np_ : (d + 1) * np_, b * LANE : (b + 1) * LANE
                ].astype(BF16)

    def rd_copy(k, side):
        kind, g = plan.sets[side][k]
        return send(
            part[kind].at[g, pl.ds((1 - c) * half, half)], got_d[kind].at[g],
            (t.rd_send, t.rd_recv), (k, side), {"batch": plan.batch(1 - c, m, z)},
        )

    def rm_copy(k, j, jx, chunk):
        kind, g = chunk
        to = (m + j) % nm
        return send(
            two[kind].at[g, pl.ds(to * nz, nz)], got_m[kind].at[g, jx * nm + j - 1],
            (t.rm_send, t.rm_recv), (k, jx * nm + j - 1),
            {"batch": plan.batch(c, to, z), "rows": (r + jx) % 2},
        )

    def step_m(k):
        for side in range(2):
            rd_copy(k, side).wait()

        def fn(rr):
            for j, jx in peers:
                kind, g = plan.sets[(rr + jx) % 2][k]
                first = (m + j) % nm * nz
                two[kind][g, pl.ds(first, nz)] = (
                    part[kind][g, pl.ds(c * half + first, nz)] + got_d[kind][g, pl.ds(first, nz)]
                )
                rm_copy(k, j, jx, (kind, g)).start()
        by_half(r, fn)

    def rz_copy(k, j, chunk):
        kind, g = chunk
        to = (z + j) % nz
        return send(
            eight[kind].at[g, to], got_z[kind].at[g, j - 1],
            (t.rz_send, t.rz_recv), (k, j - 1), {"batch": plan.batch(c, m, to)},
        )

    def sum_m(kind, g, at):
        first = m * nz + at
        total = part[kind][g, c * half + first].astype(F32) + got_d[kind][g, first].astype(F32)
        for i in range(2 * nm - 1):
            total = total + got_m[kind][g, i, at].astype(F32)
        return total

    def step_z(k):
        def fn(rr):
            for j, jx in peers:
                rm_copy(k, j, jx, plan.sets[(rr + jx) % 2][k]).wait_send()
                rm_copy(k, j, jx, plan.sets[rr][k]).wait_recv()
            kind, g = plan.sets[rr][k]
            for j in range(1, nz):
                to = (z + j) % nz
                eight[kind][g, to] = sum_m(kind, g, to).astype(BF16)
                rz_copy(k, j, (kind, g)).start()
            grads[kind][g] = sum_m(kind, g, z)
        by_half(r, fn)

    def x_copy(k, chunk):
        kind, g = chunk
        return send(grads[kind].at[g], grads[kind].at[g], (t.x_send, t.x_recv), k, {"rows": 1 - r})

    lead = plan.lead
    chip = m * nz + z

    def swap(k):
        return send(t.src2.at[k], t.other.at[k], (t.c_send, t.c_recv), k, {"batch": plan.batch(1 - c, m, z)})

    def finish(k):
        def fn(rr):
            kind, g = plan.sets[rr][k]
            total = grads[kind][g]
            for j in range(1, nz):
                rz_copy(k, j, (kind, g)).wait()
                total = total + got_z[kind][g, j - 1].astype(F32)
            total = total / images
            grads[kind][g] = total
            for b, (which, col) in enumerate(plan.tiles_of((kind, g))):
                count = plan.count_of(which)
                i = plan.starts[rr][k] + b
                piece = total[b * count : (b + 1) * count]
                cent = w_refs[which][:, col : col + LANE] - t.stat[rr, i : i + 1]
                s = jnp.sum(piece, axis=0, keepdims=True)
                off = piece - s / count
                t.src2[k, b : b + 1] = s
                t.src2[k, lead + b : lead + b + 1] = jnp.sum(off * off, axis=0, keepdims=True)
                t.src2[k, 2 * lead + b : 2 * lead + b + 1] = jnp.sum(piece * cent, axis=0, keepdims=True)
            swap(k).start()
            if k != order[-1]:
                x_copy(k, (kind, g)).start()
        by_half(r, fn)

    def count_at(rr, k):
        return float(plan.nc if plan.sets[rr][k][0] == "c" else plan.np_)

    def stat_copies(k):
        return [
            send(
                t.both.at[k], t.slots2.at[k, r, chip], (t.s2_send, t.s2_recv), (k, jx * half + d - 1),
                {"batch": (me + 2 * d) % n, "rows": (r + jx) % 2},
            )
            for jx in (1, 0) for d in range(half) if (d, jx) != (0, 0)
        ]

    def share(k):
        swap(k).wait()
        total, _, between = merged([t.src2[k], t.other[k]], jnp.where(r == 0, count_at(0, k), count_at(1, k)))
        t.both[k] = total
        t.both[k, lead : 2 * lead] = total[lead : 2 * lead] + between[0:lead]
        for copy in stat_copies(k):
            copy.start()
        t.slots2[k, r, chip] = t.both[k]

    def coefs(k):
        for copy in stat_copies(k):
            copy.wait()
        for rr in range(2):
            count = count_at(rr, k)
            many = len(plan.tiles_of(plan.sets[rr][k]))
            at = plan.starts[rr][k]
            total, gmean, between = merged([t.slots2[k, rr, i] for i in range(half)], 2.0 * count)
            gspread = total[lead : lead + many] + between[0:many]
            proj = total[2 * lead : 2 * lead + many]
            mean = t.stat[rr, at : at + many]
            spread = t.stat[rr, 8 + at : 8 + at + many]
            factor = lax.rsqrt(spread + ws_eps)
            f2 = factor * factor
            one = t.gain[rr, at : at + many] * factor
            coef_two = one * f2 * proj
            grad_sq = one * one * jnp.maximum(gspread - f2 * proj * proj * (2.0 - f2 * spread), 0.0)
            weight_sq = spread + n * count * (mean * mean)
            clip = jnp.minimum(1.0, clip_ratio * jnp.sqrt(weight_sq) * lax.rsqrt(grad_sq + norm_eps))
            t.coef[rr, at : at + many] = clip * one
            t.coef[rr, 8 + at : 8 + at + many] = gmean[0:many]
            t.coef[rr, 16 + at : 16 + at + many] = clip * coef_two

    order = list(reversed(range(plan.pieces)))
    before = None
    for k in order:
        for side in range(2):
            produce(plan.sets[side][k])
            rd_copy(k, side).start()
        if before is not None:
            step_m(before)
        before = k
    step_m(before)

    tall = next(k for k in (2, 1) if mr % k == 0)

    def back(s, carry):
        at = pl.multiple_of(s * tall * mc, mc)
        for g in range(groups):
            acc = None
            for i in range(TAPS):
                for j in range(TAPS):
                    term = dot_nt(
                        t.ys[pl.ds(pl.multiple_of(at + (2 - i) * mc, mc), tall * mc), g * wide + j * gw : g * wide + (j + 1) * gw],
                        t.kt[i * wide + j * gw : i * wide + (j + 1) * gw, g * gw : (g + 1) * gw],
                    )
                    acc = term if acc is None else acc + term
            slope = gelu_parts(t.x[pl.ds(at, tall * mc), g * gw : (g + 1) * gw].astype(F32))[1]
            t.ig[pl.ds(at, tall * mc), g * gw : (g + 1) * gw] = (acc * slope).astype(BF16)
        return carry

    lax.fori_loop(0, mr // tall, back, 0)
    for k in order:
        step_z(k)
    t.src2[...] = jnp.zeros_like(t.src2)
    ahead = []
    for k in order:
        finish(k)
        if len(ahead) == 2:
            share(ahead.pop(0))
        ahead.append(k)
    for k in ahead:
        share(k)

    def last_x(rr):
        x_copy(order[-1], plan.sets[rr][order[-1]]).start()

    by_half(r, last_x)
    halos[2].wait()
    for k in order:
        coefs(k)

    def end(rr):
        for k in range(plan.pieces):
            x_copy(k, plan.sets[rr][k]).wait_send()
            x_copy(k, plan.sets[1 - rr][k]).wait_recv()

    by_half(r, end)


def update_kernel(plan, gradc_ref, gradq_ref, coef_ref, stat_ref, wc_ref, wp_ref, mc_ref, mp_ref, ig_in,
                  nwc_ref, nwp_ref, nmc_ref, nmp_ref, ig_out, sem):
    store = pltpu.make_async_copy(ig_in, ig_out, sem)
    store.start()
    grads = {"c": gradc_ref, "q": gradq_ref}
    for rr in range(2):
        i = 0
        for chunk in plan.sets[rr]:
            kind, g = chunk
            for b, (which, col) in enumerate(plan.tiles_of(chunk)):
                count = plan.count_of(which)
                cols = slice(col, col + LANE)
                w = (wc_ref, wp_ref)[which][:, cols]
                grad = grads[kind][g, b * count : (b + 1) * count]
                clipped = coef_ref[rr, i : i + 1] * (grad - coef_ref[rr, 8 + i : 9 + i]) - coef_ref[
                    rr, 16 + i : 17 + i
                ] * (w - stat_ref[rr, i : i + 1])
                new_m = momentum_rate * (mc_ref, mp_ref)[which][:, cols] + clipped
                (nmc_ref, nmp_ref)[which][:, cols] = new_m
                (nwc_ref, nwp_ref)[which][:, cols] = w - learn_rate * (clipped + momentum_rate * new_m)
                i += 1
    store.wait()


main_vmem = 40 * 2**20
update_vmem = 8 * 2**20


def local(n, nrows, block_input, output_grad, conv_weight, conv_gain, conv_momentum,
          proj_weight, proj_gain, proj_momentum):
    assert nrows == 2
    _, mr, mc, ch = block_input.shape
    out = output_grad.shape[3]
    nc = conv_weight.shape[1]
    np_ = proj_weight.shape[1]
    gw = nc * n // (TAPS * TAPS)
    assert gw == LANE
    plan = Plan(n, ch, out, nc, np_)
    nz, nm, half, pieces = plan.nz, plan.nm, plan.half, plan.pieces
    px = mr * mc
    rq = plan.chunk_rows("q")

    wc, wp, mc_, mp = conv_weight.T, proj_weight.T, conv_momentum.T, proj_momentum.T
    gc, gp = conv_gain, proj_gain
    x = block_input.reshape(px, ch)
    u = output_grad.reshape(px, out)
    wc, wp, gc, gp, x, u = (pltpu.with_memory_space_constraint(a, pltpu.HBM) for a in (wc, wp, gc, gp, x, u))
    vmem = pl.BlockSpec(memory_space=pltpu.VMEM)
    sdt = jax.ShapeDtypeStruct
    dma = pltpu.SemaphoreType.DMA
    scratch = {}

    def pair(name, shape):
        scratch[name + "_send"] = dma(shape)
        scratch[name + "_recv"] = dma(shape)

    def both(name, *lead):
        scratch[name + "c"] = pltpu.VMEM((pieces, *lead, nc, LANE), BF16)
        scratch[name + "q"] = pltpu.VMEM((pieces, *lead, rq, LANE), BF16)

    scratch.update(
        x=pltpu.VMEM((px, ch), BF16),
        u=pltpu.VMEM((px, out), BF16),
        gc=pltpu.VMEM((ch,), F32),
        gp=pltpu.VMEM((out,), F32),
        hx=pltpu.VMEM((2 * mc, ch), BF16),
        hu=pltpu.VMEM((mc, out), BF16),
        kt=pltpu.VMEM((n * nc, ch), BF16),
        pt=pltpu.VMEM((n * np_, out), BF16),
        xs=pltpu.VMEM(((mr + 4) * mc, TAPS * ch), BF16),
        ys=pltpu.VMEM(((mr + 2) * mc, TAPS * ch), BF16),
        hid=pltpu.VMEM(((mr + 2) * mc, ch), BF16),
        cg=pltpu.VMEM((n * nc, LANE), F32),
        pg=pltpu.VMEM((n * np_, plan.nblk * LANE), F32),
        src=pltpu.VMEM((2, 8, LANE), F32),
        slots=pltpu.VMEM((2, n, 8, LANE), F32),
        src2=pltpu.VMEM((pieces, 8, LANE), F32),
        other=pltpu.VMEM((pieces, 8, LANE), F32),
        both=pltpu.VMEM((pieces, 8, LANE), F32),
        slots2=pltpu.VMEM((pieces, 2, half, 8, LANE), F32),
        gain=pltpu.VMEM((2, 8, LANE), F32),
        load=dma((6,)),
    )
    for name, lead in (("f", (n,)), ("p", (n,)), ("gd", (half,)), ("two", (half,)),
                       ("gm", (2 * nm - 1, nz)), ("eight", (nz,)), ("gz", (max(nz - 1, 1),))):
        both(name, *lead)
    pair("s", (2, n - 1))
    pair("s2", (pieces, n - 1))
    pair("c", (pieces,))
    for name in ("z", "rz"):
        pair(name, (pieces, max(nz - 1, 1)))
    for name in ("m", "rm"):
        pair(name, (pieces, 2 * nm - 1))
    for name in ("d", "rd"):
        pair(name, (pieces, 2))
    pair("h", (3,))
    pair("x", (pieces + 1,))
    names = ["wc_any", "wp_any", "gc_any", "gp_any", "x_any", "u_any", "ig", "gradc", "gradq", "coef", "stat", "wc", "wp", *scratch]
    ig, gradc, gradq, coef, stat, wc, wp = pl.pallas_call(
        functools.partial(main_kernel, plan, names, mr, mc, gw, n),
        out_shape=(
            sdt((px, ch), BF16),
            sdt((pieces, nc, LANE), F32),
            sdt((pieces, rq, LANE), F32),
            sdt((2, 24, LANE), F32),
            sdt((2, 16, LANE), F32),
            sdt((nc, ch), F32),
            sdt((np_, out), F32),
        ),
        in_specs=[pl.BlockSpec(memory_space=pltpu.HBM)] * 6,
        out_specs=(vmem,) * 7,
        scratch_shapes=list(scratch.values()),
        compiler_params=pltpu.CompilerParams(
            collective_id=0, has_side_effects=True, vmem_limit_bytes=main_vmem
        ),
        name="main",
    )(wc, wp, gc, gp, x, u)
    nwc, nwp, nmc, nmp, ig = pl.pallas_call(
        functools.partial(update_kernel, plan),
        out_shape=(sdt((nc, ch), F32), sdt((np_, out), F32)) * 2 + (sdt((px, ch), BF16),),
        in_specs=[vmem] * 9,
        out_specs=(vmem,) * 4 + (pl.BlockSpec(memory_space=pl.ANY),),
        scratch_shapes=[dma],
        compiler_params=pltpu.CompilerParams(vmem_limit_bytes=update_vmem),
        name="update",
    )(gradc, gradq, coef, stat, wc, wp, mc_, mp, ig)
    return (ig.reshape(block_input.shape), nwc.T, nmc.T, nwp.T, nmp.T)


def solution(mesh):
    in_specs = (
        P("batch", "rows", None, None),
        P("batch", "rows", None, None),
        P(None, "batch"),
        P(),
        P(None, "batch"),
        P(None, "batch"),
        P(),
        P(None, "batch"),
    )
    out_specs = (
        P("batch", "rows", None, None),
        P(None, "batch"),
        P(None, "batch"),
        P(None, "batch"),
        P(None, "batch"),
    )
    body = functools.partial(local, mesh.shape["batch"], mesh.shape["rows"])
    return jax.shard_map(body, mesh=mesh, in_specs=in_specs, out_specs=out_specs, check_vma=False)
```

```python
import functools
import math

import jax
import jax.numpy as jnp
from jax import lax
from jax.experimental import pallas as pl
from jax.experimental.pallas import tpu as pltpu
from jax.sharding import PartitionSpec as P

ws_eps = 0.0001
clip_ratio = 0.05
momentum_rate = 0.9
learn_rate = 1.6
norm_eps = 1e-06

F32 = jnp.float32
BF16 = jnp.bfloat16
MESH = pl.DeviceIdType.MESH
TAPS = 3
C0 = math.sqrt(2.0 / math.pi)
C1 = 0.044715


def gelu_parts(x):
    t = jnp.tanh(C0 * (x + C1 * (x * x * x)))
    half = 0.5 * (1.0 + t)
    slope = half + (0.5 * C0) * x * (1.0 - t * t) * (1.0 + (3.0 * C1) * (x * x))
    return x * half, slope


def dot_nn(a, b):
    return jnp.dot(a, b, preferred_element_type=F32)


def dot_nt(a, b):
    return lax.dot_general(a, b, (((1,), (1,)), ((), ())), preferred_element_type=F32)


def dot_tn(a, b):
    return lax.dot_general(a, b, (((0,), (0,)), ((), ())), preferred_element_type=F32)


LANE = 128


class Plan:
    def __init__(self, n, ch, out, nc, np_):
        nb = n.bit_length() - 1
        assert 2**nb == n and nb >= 1
        self.n, self.nc, self.np_ = n, nc, np_
        self.nz = 2 ** (nb // 2)
        self.nm = n // 2 // self.nz
        self.half = n // 2
        self.ch, self.out = ch, out
        self.nblk = out // ch
        self.pieces = ch // LANE
        cut = self.pieces // 2
        rest = self.pieces - cut
        self.sets = (
            [("q", k) for k in range(cut)] + [("c", k) for k in range(rest)],
            [("q", k) for k in range(cut, self.pieces)] + [("c", k) for k in range(rest, self.pieces)],
        )
        self.tiles = tuple([t for chunk in one for t in self.tiles_of(chunk)] for one in self.sets)
        self.lead = self.nblk
        self.wide = max(len(t) for t in self.tiles)
        assert cut and self.wide <= 8 and self.wide - self.lead <= 4
        self.starts = tuple(
            [sum(len(self.tiles_of(chunk)) for chunk in one[:k]) for k in range(self.pieces)] for one in self.sets
        )

    def tiles_of(self, chunk):
        kind, k = chunk
        if kind == "c":
            return [(0, k * LANE)]
        return [(1, b * self.ch + k * LANE) for b in range(self.nblk)]

    def count_of(self, which):
        return self.np_ if which else self.nc

    def chunk_rows(self, kind):
        return self.nc if kind == "c" else self.nblk * self.np_

    def slot(self, d):
        return (d % 2 * self.nm + d // 2 % self.nm) * self.nz + d // 2 // self.nm

    def place(self, me):
        return me % 2, me // 2 % self.nm, me // 2 // self.nm

    def batch(self, c, m, z):
        return (z * self.nm + m) * 2 + c


def send(src, dst, sems, at, where):
    return pltpu.make_async_remote_copy(
        src_ref=src, dst_ref=dst, send_sem=sems[0].at[at], recv_sem=sems[1].at[at],
        device_id=where, device_id_type=MESH,
    )


def greet(plan):
    me = lax.axis_index("batch")
    r = lax.axis_index("rows")
    n = plan.n
    barrier = pltpu.get_barrier_semaphore()
    for d in range(1, n):
        pl.semaphore_signal(barrier, inc=1, device_id={"batch": (me + d) % n}, device_id_type=MESH)
    for d in range(plan.half):
        to = (me + 2 * d) % n
        pl.semaphore_signal(barrier, inc=1, device_id={"batch": to, "rows": 1 - r}, device_id_type=MESH)


def greet_wait(plan):
    pl.semaphore_wait(pltpu.get_barrier_semaphore(), plan.n - 1 + plan.half)


def merged(entries, cnt):
    total = entries[0]
    for one in entries[1:]:
        total = total + one
    mean = total / (len(entries) * cnt)
    between = None
    for one in entries:
        off = one / cnt - mean
        term = cnt * (off * off)
        between = term if between is None else between + term
    return total, mean, between


def by_half(r, fn):
    for rr in range(2):
        @pl.when(r == rr)
        def _(rr=rr):
            fn(rr)


def shifted(vals, step, mc):
    rows = vals.shape[0]
    col = lax.broadcasted_iota(jnp.int32, vals.shape, 0)
    if step > 0:
        return jnp.where(col == mc - 1, 0.0, pltpu.roll(vals, rows - 1, 0))
    return jnp.where(col == 0, 0.0, pltpu.roll(vals, 1, 0))


class Refs:
    pass


def main_kernel(plan, names, mr, mc, gw, images, *refs):
    t = Refs()
    for name, ref in zip(names, refs, strict=True):
        setattr(t, name, ref)
    me = lax.axis_index("batch")
    r = lax.axis_index("rows")
    c, m, z = plan.place(me)
    n, nz, nm, half = plan.n, plan.nz, plan.nm, plan.half
    nc, np_, nblk, ch = plan.nc, plan.np_, plan.nblk, plan.ch
    groups = ch // gw
    wide = TAPS * gw
    px = mr * mc
    w_refs = (t.wc, t.wp)
    gain_refs = (t.gc, t.gp)
    full = {"c": t.fc, "q": t.fq}
    loads = []
    for at, (far, near) in enumerate(((t.wc_any, t.wc), (t.wp_any, t.wp), (t.gc_any, t.gc), (t.gp_any, t.gp),
                                      (t.x_any, t.x), (t.u_any, t.u))):
        copy = pltpu.make_async_copy(far, near, t.load.at[at])
        copy.start()
        loads.append(copy)
    greet(plan)

    t.src[...] = jnp.zeros_like(t.src)

    def weight_stats(rr):
        for i, (which, col) in enumerate(plan.tiles[rr]):
            piece = w_refs[which][:, col : col + LANE]
            s = jnp.sum(piece, axis=0, keepdims=True)
            cent = piece - s / piece.shape[0]
            late = int(i >= plan.lead)
            row = i - late * plan.lead
            t.src[late, row : row + 1] = s
            t.src[late, 4 + row : 5 + row] = jnp.sum(cent * cent, axis=0, keepdims=True)

    for copy in loads[:4]:
        copy.wait()
    by_half(r, weight_stats)
    greet_wait(plan)
    push = [[], []]
    for late in range(2):
        for d in range(1, n):
            copy = send(
                t.src.at[late], t.slots.at[late, me], (t.s_send, t.s_recv), (late, d - 1), {"batch": (me + d) % n}
            )
            copy.start()
            push[late].append(copy)
        t.slots[late, me] = t.src[late]
    halos = []
    for at, (load, ref, out) in enumerate(((loads[4], t.x, t.hx), (loads[5], t.u, t.hu))):
        load.wait()
        width = out.shape[0]
        first = (1 - r) * (ref.shape[0] - width)
        copy = send(ref.at[pl.ds(first, width)], out, (t.h_send, t.h_recv), at, {"rows": 1 - r})
        copy.start()
        halos.append(copy)

    def place(at, vals):
        act = gelu_parts(vals)[0].astype(BF16).astype(F32)
        for j in range(TAPS):
            moved = act if j == 1 else shifted(act, j - 1, mc)
            moved = moved.astype(BF16)
            for g in range(groups):
                t.xs[pl.ds(at, mc), g * wide + j * gw : g * wide + (j + 1) * gw] = moved[
                    :, g * gw : (g + 1) * gw
                ]

    def body(row, carry):
        at = pl.multiple_of(row * mc, mc)
        place(pl.multiple_of(at + 2 * mc, mc), t.x[pl.ds(at, mc)].astype(F32))
        return carry

    lax.fori_loop(0, mr, body, 0)
    t.gain[...] = jnp.zeros_like(t.gain)
    for rr in range(2):
        for i, (which, col) in enumerate(plan.tiles[rr]):
            t.gain[rr, i : i + 1] = gain_refs[which][col : col + LANE][None]

    slot = (c * nm + m) * nz + z
    base = (c * nm + m) * nz

    def z_copy(k, j, chunk):
        kind, g = chunk
        at = full[kind].at[g, slot]
        return send(at, at, (t.z_send, t.z_recv), (k, j - 1), {"batch": plan.batch(c, m, (z + j) % nz)})

    t.stat[r] = jnp.zeros_like(t.stat[0])
    row = lax.broadcasted_iota(jnp.int32, (8, LANE), 0)
    for late in range(2):
        for copy in push[late]:
            copy.wait()
        ks = range(1, plan.pieces) if late else range(1)
        tiles = [plan.tiles[rr][plan.lead :] if late else plan.tiles[rr][: plan.lead] for rr in range(2)]
        first = [sum(which for which, _ in one) for one in tiles]
        most = max(len(one) for one in tiles)
        cnt = jnp.where(row < jnp.where(r == 0, first[0], first[1]), float(np_), float(nc))
        total, mean, between = merged([t.slots[late, i] for i in range(n)], cnt)
        spread = total[4 : 4 + most] + between[0:most]
        factor = lax.rsqrt(spread + ws_eps)
        at = late * plan.lead
        t.stat[r, at : at + most] = mean[0:most]
        t.stat[r, 8 + at : 8 + at + most] = spread

        def start_z(rr, ks=ks, mean=mean, factor=factor):
            i = 0
            for k in ks:
                kind, g = plan.sets[rr][k]
                for b, (which, col) in enumerate(plan.tiles_of((kind, g))):
                    count = plan.count_of(which)
                    scale = gain_refs[which][col : col + LANE][None] * factor[i : i + 1]
                    std = (scale * (w_refs[which][:, col : col + LANE] - mean[i : i + 1])).astype(BF16)
                    full[kind][g, slot, b * count : (b + 1) * count] = std
                    i += 1
                for j in range(1, nz):
                    z_copy(k, j, (kind, g)).start()

        by_half(r, start_z)
    copy = send(t.stat.at[r], t.stat.at[r], (t.h_send, t.h_recv), 2, {"rows": 1 - r})
    copy.start()
    halos.append(copy)

    def m_copy(k, j, jx, chunk):
        kind, g = chunk
        at = full[kind].at[g, pl.ds(base, nz)]
        where = {"batch": plan.batch(c, (m + j) % nm, z), "rows": (r + jx) % 2}
        return send(at, at, (t.m_send, t.m_recv), (k, jx * nm + j - 1), where)

    peers = [(j, jx) for jx in (1, 0) for j in reversed(range(nm)) if (j, jx) != (0, 0)]

    def spread_m(k):
        def fn(rr):
            chunk = plan.sets[rr][k]
            for j in range(1, nz):
                z_copy(k, j, chunk).wait()
            for j, jx in peers:
                m_copy(k, j, jx, chunk).start()
        by_half(r, fn)

    def finish_m(k):
        def fn(rr):
            for j, jx in peers:
                m_copy(k, j, jx, plan.sets[rr][k]).wait_send()
                m_copy(k, j, jx, plan.sets[(rr + jx) % 2][k]).wait_recv()
        by_half(r, fn)
        for side in range(2):
            d_copy(k, side).start()

    def d_copy(k, side):
        kind, g = plan.sets[side][k]
        at = full[kind].at[g, pl.ds(c * half, half)]
        return send(at, at, (t.d_send, t.d_recv), (k, side), {"batch": plan.batch(1 - c, m, z)})

    def unpack(chunk):
        kind, g = chunk
        lanes = slice(g * LANE, (g + 1) * LANE)
        for d in range(n):
            if kind == "c":
                t.kt[d * nc : (d + 1) * nc, lanes] = t.fc[g, plan.slot(d)]
                continue
            for b in range(nblk):
                t.pt[d * np_ : (d + 1) * np_, b * ch + g * LANE : b * ch + (g + 1) * LANE] = t.fq[
                    g, plan.slot(d), b * np_ : (b + 1) * np_
                ]

    def forward(g, e, up):
        rows = up.shape[0]
        hg = dot_nt(up, t.pt[g * gw : (g + 1) * gw])
        acc = None
        for i in range(TAPS):
            term = dot_nn(
                t.xs[pl.ds(pl.multiple_of((e + i) * mc, mc), rows), g * wide : (g + 1) * wide],
                t.kt[i * wide : (i + 1) * wide, g * gw : (g + 1) * gw],
            )
            acc = term if acc is None else acc + term
        h, slope = gelu_parts(acc)
        t.hid[pl.ds(pl.multiple_of(e * mc, mc), rows), g * gw : (g + 1) * gw] = h.astype(BF16)
        grad = (hg * slope).astype(BF16).astype(F32)
        for q in range(rows // mc):
            here = grad[q * mc : (q + 1) * mc]
            for j in range(TAPS):
                moved = here if j == 1 else shifted(here, 1 - j, mc)
                t.ys[pl.ds(pl.multiple_of((e + q) * mc, mc), mc), g * wide + j * gw : g * wide + (j + 1) * gw] = moved.astype(BF16)

    many = next(k for k in (8, 4, 2, 1) if mr % k == 0)

    def forward_all(g):
        forward(g, jnp.where(r == 1, 0, mr + 1), t.hu[...])

        def fwd(s, carry):
            up = t.u[pl.ds(pl.multiple_of(s * many * mc, mc), many * mc)]
            forward(g, 1 + s * many, up)
            return carry

        lax.fori_loop(0, mr // many, fwd, 0)

    halos[0].wait()
    near = pl.multiple_of(jnp.where(r == 1, 0, (mr + 2) * mc), mc)
    far = pl.multiple_of(jnp.where(r == 1, (mr + 2) * mc, 0), mc)
    t.xs[pl.ds(far, 2 * mc)] = jnp.zeros((2 * mc, t.xs.shape[1]), BF16)
    for e in range(2):
        place(pl.multiple_of(near + e * mc, mc), t.hx[e * mc : (e + 1) * mc].astype(F32))
    outside = pl.multiple_of(jnp.where(r == 1, (mr + 1) * mc, 0), mc)
    t.ys[pl.ds(outside, mc)] = jnp.zeros((mc, t.ys.shape[1]), BF16)
    halos[1].wait()

    for k in range(plan.pieces):
        spread_m(k)

    part = {"c": t.pc, "q": t.pq}
    got_d = {"c": t.gdc, "q": t.gdq}
    two = {"c": t.twoc, "q": t.twoq}
    got_m = {"c": t.gmc, "q": t.gmq}
    eight = {"c": t.eightc, "q": t.eightq}
    got_z = {"c": t.gzc, "q": t.gzq}
    grads = {"c": t.gradc, "q": t.gradq}

    def produce(chunk):
        kind, g = chunk
        if kind == "c":
            own = t.ys[mc : mc + px, g * wide + gw : g * wide + 2 * gw]
            for i in range(TAPS):
                t.cg[i * wide : (i + 1) * wide] = dot_tn(
                    t.xs[(1 + i) * mc : (1 + i) * mc + px, g * wide : (g + 1) * wide], own
                )
            for d in range(n):
                t.pc[g, plan.slot(d)] = t.cg[d * nc : (d + 1) * nc].astype(BF16)
            return
        for b in range(nblk):
            at = b * ch + g * LANE
            t.pg[:, b * LANE : (b + 1) * LANE] = dot_tn(t.hid[mc : mc + px], t.u[:, at : at + LANE])
        for d in range(n):
            for b in range(nblk):
                t.pq[g, plan.slot(d), b * np_ : (b + 1) * np_] = t.pg[
                    d * np_ : (d + 1) * np_, b * LANE : (b + 1) * LANE
                ].astype(BF16)

    def rd_copy(k, side):
        kind, g = plan.sets[side][k]
        return send(
            part[kind].at[g, pl.ds((1 - c) * half, half)], got_d[kind].at[g],
            (t.rd_send, t.rd_recv), (k, side), {"batch": plan.batch(1 - c, m, z)},
        )

    def rm_copy(k, j, jx, chunk):
        kind, g = chunk
        to = (m + j) % nm
        return send(
            two[kind].at[g, pl.ds(to * nz, nz)], got_m[kind].at[g, jx * nm + j - 1],
            (t.rm_send, t.rm_recv), (k, jx * nm + j - 1),
            {"batch": plan.batch(c, to, z), "rows": (r + jx) % 2},
        )

    def step_m(k, side):
        rd_copy(k, side).wait()
        kind, g = plan.sets[side][k]

        def fn(rr):
            for j, jx in peers:
                if (rr + jx) % 2 != side:
                    continue
                first = (m + j) % nm * nz
                two[kind][g, pl.ds(first, nz)] = (
                    part[kind][g, pl.ds(c * half + first, nz)] + got_d[kind][g, pl.ds(first, nz)]
                )
                rm_copy(k, j, jx, (kind, g)).start()
        by_half(r, fn)

    def rz_copy(k, j, chunk):
        kind, g = chunk
        to = (z + j) % nz
        return send(
            eight[kind].at[g, to], got_z[kind].at[g, j - 1],
            (t.rz_send, t.rz_recv), (k, j - 1), {"batch": plan.batch(c, m, to)},
        )

    def sum_m(kind, g, at):
        first = m * nz + at
        total = part[kind][g, c * half + first].astype(F32) + got_d[kind][g, first].astype(F32)
        for i in range(2 * nm - 1):
            total = total + got_m[kind][g, i, at].astype(F32)
        return total

    def step_z(s):
        def fn(rr):
            k = turn[rr][s]
            for j, jx in peers:
                rm_copy(k, j, jx, plan.sets[(rr + jx) % 2][k]).wait_send()
                rm_copy(k, j, jx, plan.sets[rr][k]).wait_recv()
            kind, g = plan.sets[rr][k]
            for j in range(1, nz):
                to = (z + j) % nz
                eight[kind][g, to] = sum_m(kind, g, to).astype(BF16)
                rz_copy(k, j, (kind, g)).start()
            grads[kind][g] = sum_m(kind, g, z)
        by_half(r, fn)

    def x_copy(k, chunk):
        kind, g = chunk
        return send(grads[kind].at[g], grads[kind].at[g], (t.x_send, t.x_recv), k, {"rows": 1 - r})

    lead = plan.lead
    chip = m * nz + z

    def swap(k):
        return send(t.src2.at[k], t.other.at[k], (t.c_send, t.c_recv), k, {"batch": plan.batch(1 - c, m, z)})

    def finish(nth):
        def fn(rr):
            k = turn[rr][nth]
            kind, g = plan.sets[rr][k]
            total = grads[kind][g]
            for j in range(1, nz):
                rz_copy(k, j, (kind, g)).wait()
                total = total + got_z[kind][g, j - 1].astype(F32)
            total = total / images
            grads[kind][g] = total
            for b, (which, col) in enumerate(plan.tiles_of((kind, g))):
                count = plan.count_of(which)
                i = plan.starts[rr][k] + b
                piece = total[b * count : (b + 1) * count]
                cent = w_refs[which][:, col : col + LANE] - t.stat[rr, i : i + 1]
                s = jnp.sum(piece, axis=0, keepdims=True)
                off = piece - s / count
                t.src2[k, b : b + 1] = s
                t.src2[k, lead + b : lead + b + 1] = jnp.sum(off * off, axis=0, keepdims=True)
                t.src2[k, 2 * lead + b : 2 * lead + b + 1] = jnp.sum(piece * cent, axis=0, keepdims=True)
            swap(k).start()
            if nth < plan.pieces - 1:
                x_copy(k, (kind, g)).start()
        by_half(r, fn)

    def count_at(rr, k):
        return float(plan.nc if plan.sets[rr][k][0] == "c" else plan.np_)

    def stat_copies(k):
        return [
            send(
                t.both.at[k], t.slots2.at[k, r, chip], (t.s2_send, t.s2_recv), (k, jx * half + d - 1),
                {"batch": (me + 2 * d) % n, "rows": (r + jx) % 2},
            )
            for jx in (1, 0) for d in range(half) if (d, jx) != (0, 0)
        ]

    def share(k):
        swap(k).wait()
        total, _, between = merged([t.src2[k], t.other[k]], jnp.where(r == 0, count_at(0, k), count_at(1, k)))
        t.both[k] = total
        t.both[k, lead : 2 * lead] = total[lead : 2 * lead] + between[0:lead]
        for copy in stat_copies(k):
            copy.start()
        t.slots2[k, r, chip] = t.both[k]

    def coefs(k):
        for copy in stat_copies(k):
            copy.wait()
        for rr in range(2):
            count = count_at(rr, k)
            many = len(plan.tiles_of(plan.sets[rr][k]))
            at = plan.starts[rr][k]
            total, gmean, between = merged([t.slots2[k, rr, i] for i in range(half)], 2.0 * count)
            gspread = total[lead : lead + many] + between[0:many]
            proj = total[2 * lead : 2 * lead + many]
            mean = t.stat[rr, at : at + many]
            spread = t.stat[rr, 8 + at : 8 + at + many]
            factor = lax.rsqrt(spread + ws_eps)
            f2 = factor * factor
            one = t.gain[rr, at : at + many] * factor
            coef_two = one * f2 * proj
            grad_sq = one * one * jnp.maximum(gspread - f2 * proj * proj * (2.0 - f2 * spread), 0.0)
            weight_sq = spread + n * count * (mean * mean)
            clip = jnp.minimum(1.0, clip_ratio * jnp.sqrt(weight_sq) * lax.rsqrt(grad_sq + norm_eps))
            t.coef[rr, at : at + many] = clip * one
            t.coef[rr, 8 + at : 8 + at + many] = gmean[0:many]
            t.coef[rr, 16 + at : 16 + at + many] = clip * coef_two

    made, waiting = [], []

    def drain():
        while waiting:
            step_m(*waiting.pop(0))

    def make(k, side):
        produce(plan.sets[side][k])
        rd_copy(k, side).start()
        drain()
        waiting.append((k, side))
        made.append((k, side))

    filled = []
    for k in range(plan.pieces):
        finish_m(k)
        drain()
        if k == 0:
            continue
        for q in range(k - 1, k + 1 if k == plan.pieces - 1 else k):
            for side in range(2):
                d_copy(q, side).wait()
                unpack(plan.sets[side][q])
                filled.append((q, side))
            if sum(plan.sets[side][q][0] == "q" for q, side in filled) == plan.pieces:
                for q, side in reversed(filled):
                    kind, g = plan.sets[side][q]
                    if kind == "c" and (q, side) not in made:
                        forward_all(g)
                        make(q, side)
    assert len(made) == groups
    for k in reversed(range(plan.pieces)):
        for side in range(2):
            if plan.sets[side][k][0] == "q":
                make(k, side)
    drain()
    turn = [[k for k, side in made if side == rr] for rr in range(2)]
    assert turn[0][-1] == turn[1][-1] == 0
    order = list(reversed(range(plan.pieces)))

    tall = next(k for k in (2, 1) if mr % k == 0)

    def back(s, carry):
        at = pl.multiple_of(s * tall * mc, mc)
        for g in range(groups):
            acc = None
            for i in range(TAPS):
                for j in range(TAPS):
                    term = dot_nt(
                        t.ys[pl.ds(pl.multiple_of(at + (2 - i) * mc, mc), tall * mc), g * wide + j * gw : g * wide + (j + 1) * gw],
                        t.kt[i * wide + j * gw : i * wide + (j + 1) * gw, g * gw : (g + 1) * gw],
                    )
                    acc = term if acc is None else acc + term
            slope = gelu_parts(t.x[pl.ds(at, tall * mc), g * gw : (g + 1) * gw].astype(F32))[1]
            t.ig[pl.ds(at, tall * mc), g * gw : (g + 1) * gw] = (acc * slope).astype(BF16)
        return carry

    lax.fori_loop(0, mr // tall, back, 0)
    for s in range(plan.pieces):
        step_z(s)
    t.src2[...] = jnp.zeros_like(t.src2)
    for s in range(plan.pieces - 1):
        finish(s)
    for k in order[:-1]:
        share(k)
    finish(plan.pieces - 1)
    share(order[-1])

    def last_x(rr):
        x_copy(order[-1], plan.sets[rr][order[-1]]).start()

    by_half(r, last_x)
    halos[2].wait()
    for k in order:
        coefs(k)

    def end(rr):
        for k in range(plan.pieces):
            x_copy(k, plan.sets[rr][k]).wait_send()
            x_copy(k, plan.sets[1 - rr][k]).wait_recv()

    by_half(r, end)


def update_kernel(plan, gradc_ref, gradq_ref, coef_ref, stat_ref, wc_ref, wp_ref, mc_ref, mp_ref, ig_in,
                  nwc_ref, nwp_ref, nmc_ref, nmp_ref, ig_out, sem):
    store = pltpu.make_async_copy(ig_in, ig_out, sem)
    store.start()
    grads = {"c": gradc_ref, "q": gradq_ref}
    for rr in range(2):
        i = 0
        for chunk in plan.sets[rr]:
            kind, g = chunk
            for b, (which, col) in enumerate(plan.tiles_of(chunk)):
                count = plan.count_of(which)
                cols = slice(col, col + LANE)
                w = (wc_ref, wp_ref)[which][:, cols]
                grad = grads[kind][g, b * count : (b + 1) * count]
                clipped = coef_ref[rr, i : i + 1] * (grad - coef_ref[rr, 8 + i : 9 + i]) - coef_ref[
                    rr, 16 + i : 17 + i
                ] * (w - stat_ref[rr, i : i + 1])
                new_m = momentum_rate * (mc_ref, mp_ref)[which][:, cols] + clipped
                (nmc_ref, nmp_ref)[which][:, cols] = new_m
                (nwc_ref, nwp_ref)[which][:, cols] = w - learn_rate * (clipped + momentum_rate * new_m)
                i += 1
    store.wait()


main_vmem = 40 * 2**20
update_vmem = 8 * 2**20


def local(n, nrows, block_input, output_grad, conv_weight, conv_gain, conv_momentum,
          proj_weight, proj_gain, proj_momentum):
    assert nrows == 2
    _, mr, mc, ch = block_input.shape
    out = output_grad.shape[3]
    nc = conv_weight.shape[1]
    np_ = proj_weight.shape[1]
    gw = nc * n // (TAPS * TAPS)
    assert gw == LANE
    plan = Plan(n, ch, out, nc, np_)
    nz, nm, half, pieces = plan.nz, plan.nm, plan.half, plan.pieces
    px = mr * mc
    rq = plan.chunk_rows("q")

    wc, wp, mc_, mp = conv_weight.T, proj_weight.T, conv_momentum.T, proj_momentum.T
    gc, gp = conv_gain, proj_gain
    x = block_input.reshape(px, ch)
    u = output_grad.reshape(px, out)
    wc, wp, gc, gp, x, u = (pltpu.with_memory_space_constraint(a, pltpu.HBM) for a in (wc, wp, gc, gp, x, u))
    vmem = pl.BlockSpec(memory_space=pltpu.VMEM)
    sdt = jax.ShapeDtypeStruct
    dma = pltpu.SemaphoreType.DMA
    scratch = {}

    def pair(name, shape):
        scratch[name + "_send"] = dma(shape)
        scratch[name + "_recv"] = dma(shape)

    def both(name, *lead):
        scratch[name + "c"] = pltpu.VMEM((pieces, *lead, nc, LANE), BF16)
        scratch[name + "q"] = pltpu.VMEM((pieces, *lead, rq, LANE), BF16)

    scratch.update(
        x=pltpu.VMEM((px, ch), BF16),
        u=pltpu.VMEM((px, out), BF16),
        gc=pltpu.VMEM((ch,), F32),
        gp=pltpu.VMEM((out,), F32),
        hx=pltpu.VMEM((2 * mc, ch), BF16),
        hu=pltpu.VMEM((mc, out), BF16),
        kt=pltpu.VMEM((n * nc, ch), BF16),
        pt=pltpu.VMEM((n * np_, out), BF16),
        xs=pltpu.VMEM(((mr + 4) * mc, TAPS * ch), BF16),
        ys=pltpu.VMEM(((mr + 2) * mc, TAPS * ch), BF16),
        hid=pltpu.VMEM(((mr + 2) * mc, ch), BF16),
        cg=pltpu.VMEM((n * nc, LANE), F32),
        pg=pltpu.VMEM((n * np_, plan.nblk * LANE), F32),
        src=pltpu.VMEM((2, 8, LANE), F32),
        slots=pltpu.VMEM((2, n, 8, LANE), F32),
        src2=pltpu.VMEM((pieces, 8, LANE), F32),
        other=pltpu.VMEM((pieces, 8, LANE), F32),
        both=pltpu.VMEM((pieces, 8, LANE), F32),
        slots2=pltpu.VMEM((pieces, 2, half, 8, LANE), F32),
        gain=pltpu.VMEM((2, 8, LANE), F32),
        load=dma((6,)),
    )
    for name, lead in (("f", (n,)), ("p", (n,)), ("gd", (half,)), ("two", (half,)),
                       ("gm", (2 * nm - 1, nz)), ("eight", (nz,)), ("gz", (max(nz - 1, 1),))):
        both(name, *lead)
    pair("s", (2, n - 1))
    pair("s2", (pieces, n - 1))
    pair("c", (pieces,))
    for name in ("z", "rz"):
        pair(name, (pieces, max(nz - 1, 1)))
    for name in ("m", "rm"):
        pair(name, (pieces, 2 * nm - 1))
    for name in ("d", "rd"):
        pair(name, (pieces, 2))
    pair("h", (3,))
    pair("x", (pieces + 1,))
    names = ["wc_any", "wp_any", "gc_any", "gp_any", "x_any", "u_any", "ig", "gradc", "gradq", "coef", "stat", "wc", "wp", *scratch]
    ig, gradc, gradq, coef, stat, wc, wp = pl.pallas_call(
        functools.partial(main_kernel, plan, names, mr, mc, gw, n),
        out_shape=(
            sdt((px, ch), BF16),
            sdt((pieces, nc, LANE), F32),
            sdt((pieces, rq, LANE), F32),
            sdt((2, 24, LANE), F32),
            sdt((2, 16, LANE), F32),
            sdt((nc, ch), F32),
            sdt((np_, out), F32),
        ),
        in_specs=[pl.BlockSpec(memory_space=pltpu.HBM)] * 6,
        out_specs=(vmem,) * 7,
        scratch_shapes=list(scratch.values()),
        compiler_params=pltpu.CompilerParams(
            collective_id=0, has_side_effects=True, vmem_limit_bytes=main_vmem
        ),
        name="main",
    )(wc, wp, gc, gp, x, u)
    nwc, nwp, nmc, nmp, ig = pl.pallas_call(
        functools.partial(update_kernel, plan),
        out_shape=(sdt((nc, ch), F32), sdt((np_, out), F32)) * 2 + (sdt((px, ch), BF16),),
        in_specs=[vmem] * 9,
        out_specs=(vmem,) * 4 + (pl.BlockSpec(memory_space=pl.ANY),),
        scratch_shapes=[dma],
        compiler_params=pltpu.CompilerParams(vmem_limit_bytes=update_vmem),
        name="update",
    )(gradc, gradq, coef, stat, wc, wp, mc_, mp, ig)
    return (ig.reshape(block_input.shape), nwc.T, nmc.T, nwp.T, nmp.T)


def solution(mesh):
    in_specs = (
        P("batch", "rows", None, None),
        P("batch", "rows", None, None),
        P(None, "batch"),
        P(),
        P(None, "batch"),
        P(None, "batch"),
        P(),
        P(None, "batch"),
    )
    out_specs = (
        P("batch", "rows", None, None),
        P(None, "batch"),
        P(None, "batch"),
        P(None, "batch"),
        P(None, "batch"),
    )
    body = functools.partial(local, mesh.shape["batch"], mesh.shape["rows"])
    return jax.shard_map(body, mesh=mesh, in_specs=in_specs, out_specs=out_specs, check_vma=False)
```
